32 devices in a mesh: parts: 1 (over z), col: 4 (over y), row: 4 (over x), sub: 2 (over core).
Axes of the slice: x: 4, y: 4, z: 1, core: 2. Of those that a mesh axis runs over, the one named last changes fastest.
The devices are a block of a 4x4x8 slice.
Arguments:
- edge_dist: float32 [8, 128, 1024], P(('parts', 'row', 'sub'), None, 'col')
Outputs:
- output: float32 [8, 128, 1024], P(('parts', 'row', 'sub'), None, 'col')
All inputs are finite; a program needn't handle non-finite values.
Results may differ from the reference program's by a relative error of at most 0.001.
Values sent between devices are 32-bit elements.
A program may use at most 768 MiB of HBM per device.

```python
import jax
import jax.numpy as jnp
from jax import lax

VERTICES = 1024
BLOCK = 128
ROW_DEVS = 8
COL_DEVS = 4
CHORDS = 2

ROUNDS = VERTICES // BLOCK
NO_EDGE = 2 ** 16


def to_stored(full_dist):
    by_rows = full_dist.reshape(ROUNDS // ROW_DEVS, ROW_DEVS, BLOCK, VERTICES).transpose(1, 0, 2, 3)
    by_rows = by_rows.reshape(ROUNDS, BLOCK, ROUNDS // COL_DEVS, COL_DEVS, BLOCK).transpose(0, 1, 3, 2, 4)
    return by_rows.reshape(ROUNDS, BLOCK, VERTICES)


def from_stored(stored):
    by_cols = stored.reshape(ROUNDS, BLOCK, COL_DEVS, ROUNDS // COL_DEVS, BLOCK).transpose(0, 1, 3, 2, 4)
    by_cols = by_cols.reshape(ROW_DEVS, ROUNDS // ROW_DEVS, BLOCK, VERTICES).transpose(1, 0, 2, 3)
    return by_cols.reshape(VERTICES, VERTICES)


def setup_inputs(seed: int = 0, part: int = 0) -> dict:
    base_key = jax.random.fold_in(jax.random.key(seed), part)
    key_cycle, key_dst, key_wt = jax.random.split(base_key, 3)
    vertex_ids = jnp.arange(VERTICES)
    cycle_wt = jax.random.randint(key_cycle, (VERTICES,), 8, 17).astype(jnp.float32) / 8.0
    chord_dst = jax.random.randint(key_dst, (VERTICES, CHORDS), 0, VERTICES)
    chord_wt = jax.random.randint(key_wt, (VERTICES, CHORDS), 1, 17).astype(jnp.float32) / 8.0
    full_dist = jnp.full((VERTICES, VERTICES), NO_EDGE, dtype=jnp.float32)
    full_dist = full_dist.at[vertex_ids, (vertex_ids + 1) % VERTICES].min(cycle_wt)
    full_dist = full_dist.at[vertex_ids[:, None], chord_dst].min(chord_wt)
    full_dist = full_dist.at[vertex_ids, vertex_ids].set(0.0)
    return {'edge_dist': to_stored(full_dist)}


def close_block(block_in):
    def pivot_step(pivot_idx, current):
        col_vec = lax.dynamic_slice_in_dim(current, pivot_idx, 1, axis=1)
        row_vec = lax.dynamic_slice_in_dim(current, pivot_idx, 1, axis=0)
        return jnp.minimum(current, col_vec + row_vec)
    return lax.fori_loop(0, block_in.shape[0], pivot_step, block_in)


def min_plus(left_mat, right_mat):
    num_rows = left_mat.shape[0]
    row_groups = left_mat.reshape(num_rows // 8, 8, left_mat.shape[1])
    result = lax.map(lambda row_group: jnp.min(row_group[:, :, None] + right_mat[None, :, :], axis=1), row_groups)
    return result.reshape(num_rows, right_mat.shape[1])


def reference(edge_dist):
    def one_round(current, round_idx):
        offset = round_idx * BLOCK
        diag_blk = close_block(lax.dynamic_slice(current, (offset, offset), (BLOCK, BLOCK)))
        row_pan = min_plus(diag_blk, lax.dynamic_slice_in_dim(current, offset, BLOCK, axis=0))
        col_pan = min_plus(lax.dynamic_slice_in_dim(current, offset, BLOCK, axis=1), diag_blk)
        return jnp.minimum(current, min_plus(col_pan, row_pan)), None
    full_dist = lax.scan(one_round, from_stored(edge_dist), jnp.arange(ROUNDS))[0]
    return to_stored(full_dist)
```

```python
import functools

import jax
import jax.numpy as jnp
from jax import lax
from jax.experimental import pallas as pl
from jax.experimental.pallas import tpu as pltpu
from jax.sharding import PartitionSpec as P

SUBL = 8
LANES = 128
CHUNK = 32


def relax(acc, src, lanes, rows):
    for n, lane in enumerate(lanes):
        acc = jnp.minimum(acc, jnp.broadcast_to(src[:, lane:lane + 1], acc.shape) + jnp.broadcast_to(rows(n), acc.shape))
    return acc


def close_tile(tile, piv_cols):
    wide = jnp.concatenate([jnp.broadcast_to(piv_cols[:, l:l + 1], (SUBL, LANES)) for l in range(SUBL)] + [tile], axis=1)
    for p in range(SUBL):
        piv, wide = wide[:, :LANES], wide[:, LANES:]
        reps = wide.shape[1] // LANES
        wide = jnp.minimum(wide, jnp.concatenate([piv] * reps, axis=1) + jnp.broadcast_to(wide[p:p + 1, :], wide.shape))
    return wide


def kernel(nrows, ncols, nsub, blk, in_ref, out_ref, work, diag_in, diag_st, colp, colp_st, rowp,
           c_send, c_recv, s_send, s_recv, r_send, r_recv, f_send, n_send, n_recv):
    x = lax.axis_index('row')
    sub = lax.axis_index('sub')
    my_col = lax.axis_index('col')
    nx = nrows // nsub
    my_row = x * nsub + sub
    nchunk = blk // CHUNK
    own = in_ref.shape[2]
    dlo = blk + own
    width = dlo + blk
    tiles = blk // SUBL
    tiles_per_chunk = CHUNK // SUBL

    def dev(row=None, col=None):
        out = {}
        if row is not None:
            out['row'] = row // nsub
            out['sub'] = row % nsub
        if col is not None:
            out['col'] = col
        return out

    def signal(target):
        pl.semaphore_signal(barrier, inc=1, device_id=target, device_id_type=pl.DeviceIdType.MESH)

    barrier = pltpu.get_barrier_semaphore()
    for d in range(1, ncols):
        signal(dev(col=(my_col + d) % ncols))
    for d in range(1, nrows):
        signal(dev(row=(my_row + d) % nrows))
    for dr in (1, nrows - 1):
        for d in range(1, ncols):
            signal(dev((my_row + dr) % nrows, (my_col + d) % ncols))
    work[:, blk:dlo] = in_ref[0]
    pl.semaphore_wait(barrier, 3 * (ncols - 1) + nrows - 1)

    def remote(src, dst, ssem, rsem, target):
        return pltpu.make_async_remote_copy(src_ref=src, dst_ref=dst, send_sem=ssem, recv_sem=rsem,
                                            device_id=target, device_id_type=pl.DeviceIdType.MESH)

    def col_copy(k, d):
        return remote(colp_st.at[k], colp.at[k], c_send.at[k, d - 1], c_recv.at[k], dev(col=(my_col + d) % ncols))

    def diag_copy(d):
        return remote(diag_st, diag_in, s_send.at[d - 1], s_recv.at[0], dev(col=(my_col + d) % ncols))

    def panel(k, a):
        lo = blk if a == nchunk - 1 else 0
        return rowp.at[k, a, :, lo:dlo]

    def row_copy(k, a, d):
        target = {'sub': (sub + 1) % nsub} if d == 0 else {'row': (x + d) % nx, 'sub': 0}
        return remote(panel(k, a), panel(k, a), r_send.at[a, d], r_recv.at[k, a], target)

    def fwd_copy(k, a):
        return remote(panel(k, a), panel(k, a), f_send.at[k, a], r_recv.at[k, a], {'sub': (sub + 1) % nsub})

    def nxt_copy(k, a, d):
        src = pl.ds(pl.multiple_of(blk + (k + 1) // ncols * blk, LANES), blk)
        return remote(rowp.at[k, a, :, src], rowp.at[k, a, :, dlo:width], n_send.at[a, d], n_recv.at[a],
                      dev(k + 1, (my_col + d) % ncols))

    def own_block(b):
        return work[:, pl.ds(pl.multiple_of(blk + b // ncols * blk, LANES), blk)]

    def send_col(k):
        @pl.when((my_col == k % ncols) & (my_row != k))
        def _():
            block = own_block(k)
            colp[k] = block
            colp_st[k] = block
            for d in range(1, ncols):
                col_copy(k, d).start()

    def send_diag():
        block = own_block(my_row)
        work[:, dlo:width] = block
        diag_st[...] = block
        for d in range(1, ncols):
            diag_copy(d).start()

    def recv_diag():
        @pl.when(my_col != my_row % ncols)
        def _():
            diag_copy(1).wait_recv()
            work[:, dlo:width] = diag_in[...]

    @pl.when((my_row <= 1) & (my_col == my_row % ncols))
    def _():
        send_diag()
    send_col(0)

    def apply_rows(lo, hi, lane_lo, k, a, count, step):
        def body(it, carry):
            r = pl.ds(pl.multiple_of(it * step, step), step)
            rows = lambda n: rowp[k, a, n:n + 1, lo:hi]
            src = work[r, lane_lo:lane_lo + blk]
            work[r, lo:hi] = relax(work[r, lo:hi], src, [a * CHUNK + l for l in range(CHUNK)], rows)
            return carry
        lax.fori_loop(0, count // step, body, 0)

    def own_turn(k):
        lo, hi, dl = blk, width, dlo - blk
        load = lambda t, n=1: work[t * SUBL:(t + n) * SUBL, lo:hi]
        piv = lambda v, g: v[:, dl + g * SUBL:dl + (g + 1) * SUBL]
        cur = close_tile(load(0), piv(load(0), 0))
        for g in range(tiles):
            a = g // tiles_per_chunk
            rows = lambda n: cur[n:n + 1, :]
            if g + 1 < tiles:
                nxt = load(g + 1)
                nxt = relax(nxt, piv(nxt, g), range(SUBL), rows)
                nxt = close_tile(nxt, piv(nxt, g + 1))
            spans = [(a * tiles_per_chunk, g), (g + 2, tiles)]
            for first, last in spans:
                for t in range(first, last, 4):
                    n = min(4, last - t)
                    vals = load(t, n)
                    work[t * SUBL:(t + n) * SUBL, lo:hi] = relax(vals, piv(vals, g), range(SUBL), rows)
            work[g * SUBL:(g + 1) * SUBL, lo:hi] = cur
            if g + 1 < tiles:
                cur = nxt
            if (g + 1) % tiles_per_chunk == 0:
                r = slice(a * CHUNK, (a + 1) * CHUNK)
                rowp[k, a, :, 0:blk] = work[r, dlo:width]
                rowp[k, a, :, blk:dlo] = work[r, blk:dlo]
                rowp[k, a, :, dlo:width] = work[r, dlo:width]
                @pl.when((k + 1 < nrows) & (my_col == (k + 1) % ncols))
                def _():
                    for d in (1, 0) + tuple(range(ncols - 1, 1, -1)):
                        nxt_copy(k, a, d).start()
                for d in (1, 0, nx - 1) + tuple(range(2, nx - 1)):
                    row_copy(k, a, d).start()
        for a in range(1, nchunk):
            apply_rows(blk, width, dlo, k, a, a * CHUNK, CHUNK)

    def other_turn(k, is_next):
        for a in range(nchunk):
            fwd_copy(k, a).wait_recv()

            @pl.when((sub == 0) & (x != k // nsub))
            def _():
                fwd_copy(k, a).start()
            if is_next:
                nxt_copy(k, a, 0).wait_recv()
            apply_rows(0 if a < nchunk - 1 else blk, width if is_next else dlo, 0, k, a, blk, 64)

    def round_body(k, carry):
        @pl.when(my_row == k)
        def _():
            @pl.when(k == 0)
            def _():
                recv_diag()
            own_turn(k)

        @pl.when(my_row != k)
        def _():
            @pl.when(my_col != k % ncols)
            def _():
                col_copy(k, 1).wait_recv()
            work[:, 0:blk] = colp[k]

            @pl.when(my_row == k + 1)
            def _():
                recv_diag()
                other_turn(k, True)

            @pl.when(my_row != k + 1)
            def _():
                other_turn(k, False)

        @pl.when(k + 1 < nrows)
        def _():
            send_col(k + 1)

        @pl.when((my_row == k + 2) & (my_col == my_row % ncols))
        def _():
            send_diag()
        return carry

    lax.fori_loop(0, nrows, round_body, 0)

    out_ref[0] = work[:, blk:dlo]

    @pl.when(my_col == my_row % ncols)
    def _():
        for d in range(1, ncols):
            diag_copy(d).wait_send()

    def drain(k, carry):
        @pl.when((my_col == k % ncols) & (my_row != k))
        def _():
            for d in range(1, ncols):
                col_copy(k, d).wait_send()

        @pl.when((sub == 0) & (x != k // nsub))
        def _():
            for a in range(nchunk):
                fwd_copy(k, a).wait_send()
        return carry
    lax.fori_loop(0, nrows, drain, 0)
    for a in range(nchunk):
        for d in range(nx):
            row_copy(my_row, a, d).wait_send()

    @pl.when((my_row + 1 < nrows) & (my_col == (my_row + 1) % ncols))
    def _():
        for a in range(nchunk):
            for d in range(ncols):
                nxt_copy(my_row, a, d).wait_send()


def solution(mesh):
    nsub = mesh.shape['sub']
    nrows = mesh.shape['row'] * nsub
    ncols = mesh.shape['col']
    dist_spec = P(('parts', 'row', 'sub'), None, 'col')

    def local_run(local):
        rows_local, blk, own = local.shape
        assert rows_local == 1
        nchunk = blk // CHUNK
        nx = nrows // nsub
        dma = pltpu.SemaphoreType.DMA
        vmem = lambda *s: pltpu.VMEM(s, jnp.float32)
        return pl.pallas_call(
            functools.partial(kernel, nrows, ncols, nsub, blk),
            out_shape=jax.ShapeDtypeStruct(local.shape, local.dtype),
            in_specs=[pl.BlockSpec(memory_space=pltpu.VMEM)],
            out_specs=pl.BlockSpec(memory_space=pltpu.VMEM),
            scratch_shapes=[
                vmem(blk, own + 2 * blk), vmem(blk, blk), vmem(blk, blk),
                vmem(nrows, blk, blk), vmem(nrows, blk, blk),
                vmem(nrows, nchunk, CHUNK, own + 2 * blk),
                dma((nrows, ncols - 1)), dma((nrows,)), dma((ncols - 1,)), dma((1,)),
                dma((nchunk, nx)), dma((nrows, nchunk)), dma((nrows, nchunk)),
                dma((nchunk, ncols)), dma((nchunk,)),
            ],
            compiler_params=pltpu.CompilerParams(collective_id=0, has_side_effects=True),
        )(local)

    return jax.shard_map(local_run, mesh=mesh, in_specs=(dist_spec,), out_specs=dist_spec, check_vma=False)
```

```python
import functools

import jax
import jax.numpy as jnp
from jax import lax
from jax.experimental import pallas as pl
from jax.experimental.pallas import tpu as pltpu
from jax.sharding import PartitionSpec as P

SUBL = 8
LANES = 128
CHUNK = 32
HALVES = 2


def relax(acc, src, cols, rows):
    for n, lane in enumerate(cols):
        acc = jnp.minimum(acc, jnp.broadcast_to(src[:, lane:lane + 1], acc.shape) + jnp.broadcast_to(rows(n), acc.shape))
    return acc


def lane_bcast(tile, lane):
    return jnp.broadcast_to(tile[:, lane:lane + 1], (tile.shape[0], LANES))


def widen(x, width):
    return jnp.concatenate([x] * (width // LANES), axis=1)


def close_tile(tile, base):
    wide = jnp.concatenate([lane_bcast(tile, base + l) for l in range(SUBL)] + [tile], axis=1)
    for p in range(SUBL):
        piv, wide = wide[:, :LANES], wide[:, LANES:]
        wide = jnp.minimum(wide, widen(piv, wide.shape[1]) + jnp.broadcast_to(wide[p:p + 1, :], wide.shape))
    return wide


def kernel(nrows, ncols, nsub, blk, in_ref, out_ref, work, diag_in, colp, rowp, lanes, spread, io_sem,
           c_send, c_recv, s_send, s_recv, r_send, r_recv, f_send, n_send, n_recv):
    x = lax.axis_index('row')
    sub = lax.axis_index('sub')
    my_col = lax.axis_index('col')
    nx = nrows // nsub
    my_row = x * nsub + sub
    nchunk = blk // CHUNK
    half = blk // HALVES
    own = in_ref.shape[2]
    dlo = blk + own
    width = dlo + blk
    tiles = blk // SUBL
    tiles_per_chunk = CHUNK // SUBL

    def dev(row=None, col=None):
        out = {}
        if row is not None:
            out['row'] = row // nsub
            out['sub'] = row % nsub
        if col is not None:
            out['col'] = col
        return out

    def signal(target):
        pl.semaphore_signal(barrier, inc=1, device_id=target, device_id_type=pl.DeviceIdType.MESH)

    load_in = pltpu.make_async_copy(in_ref.at[0], work.at[:, blk:dlo], io_sem.at[0])
    load_in.start()
    barrier = pltpu.get_barrier_semaphore()
    for d in range(1, ncols):
        signal(dev(col=(my_col + d) % ncols))
    for d in range(1, nrows):
        signal(dev(row=(my_row + d) % nrows))
    for dr in (1, nrows - 1):
        for d in range(1, ncols):
            signal(dev((my_row + dr) % nrows, (my_col + d) % ncols))
    load_in.wait()
    pl.semaphore_wait(barrier, 3 * (ncols - 1) + nrows - 1)

    def remote(src, dst, ssem, rsem, target):
        return pltpu.make_async_remote_copy(src_ref=src, dst_ref=dst, send_sem=ssem, recv_sem=rsem,
                                            device_id=target, device_id_type=pl.DeviceIdType.MESH)

    def half_rows(h):
        return pl.ds(pl.multiple_of(h * half, half), half)

    def col_copy(k, h, d, n):
        part = colp.at[k, half_rows(h)]
        return remote(part, part, c_send.at[k, h, n], c_recv.at[k, h], dev(col=(my_col + d) % ncols))

    def diag_copy(h, d):
        part = diag_in.at[half_rows(h)]
        return remote(part, part, s_send.at[h, d - 1], s_recv.at[h], dev(col=(my_col + d) % ncols))

    def panel(k, a):
        lo = blk if a == nchunk - 1 else 0
        return rowp.at[k, a, :, lo:dlo]

    def row_copy(k, a, n):
        target = {'sub': (sub + 1) % nsub} if n == 0 else {'row': (x + (nx - 1, 1)[n - 1]) % nx, 'sub': 0}
        return remote(panel(k, a), panel(k, a), r_send.at[a, n], r_recv.at[k, a], target)

    def fwd_copy(k, a):
        return remote(panel(k, a), panel(k, a), f_send.at[k, a, 0], r_recv.at[k, a], {'sub': (sub + 1) % nsub})

    def far_step(a):
        return 1 if a % 2 == 0 else nx - 1

    def far_copy(k, a):
        return remote(panel(k, a), panel(k, a), f_send.at[k, a, 1], r_recv.at[k, a], {'row': (x + far_step(a)) % nx, 'sub': 0})

    def fwd_here(k):
        return (sub == 0) & (x != k // nsub)

    def far_here(k, a):
        return (sub == 0) & (x == (k // nsub + far_step(a)) % nx)

    def nxt_copy(k, a, d):
        src = pl.ds(pl.multiple_of(blk + (k + 1) // ncols * blk, LANES), blk)
        return remote(rowp.at[k, a, :, src], rowp.at[k, a, :, dlo:width], n_send.at[a, d - 1], n_recv.at[a],
                      dev(k + 1, (my_col + d) % ncols))

    def own_cols(b):
        return pl.ds(pl.multiple_of(blk + b // ncols * blk, LANES), blk)

    def send_col(k, h):
        colp[k, half_rows(h)] = work[half_rows(h), own_cols(k)]
        for d in (1, ncols - 1) + tuple(range(2, ncols - 1)):
            col_copy(k, h, d, d - 1).start()

    def send_diag(h):
        diag_in[half_rows(h)] = work[half_rows(h), own_cols(my_row)]
        work[half_rows(h), dlo:width] = diag_in[half_rows(h)]
        for d in range(1, ncols):
            diag_copy(h, d).start()

    def recv_diag():
        @pl.when(my_col != my_row % ncols)
        def _():
            for h in range(HALVES):
                diag_copy(h, 1).wait_recv()
            work[:, dlo:width] = diag_in[...]

    def recv_col(k, h):
        @pl.when(my_col != k % ncols)
        def _():
            col_copy(k, h, 1, 0).wait_recv()
        work[half_rows(h), 0:blk] = colp[k, half_rows(h)]

    @pl.when((my_row <= 1) & (my_col == my_row % ncols))
    def _():
        for h in range(HALVES):
            send_diag(h)

    @pl.when((my_row != 0) & (my_col == 0))
    def _():
        for h in range(HALVES):
            send_col(0, h)

    def apply_rows(lo, hi, lane_lo, k, a, count, step):
        def body(it, carry):
            r = pl.ds(pl.multiple_of(it * step, step), step)
            rows = lambda n: rowp[k, a, n:n + 1, lo:hi]
            src = work[r, lane_lo:lane_lo + blk]
            work[r, lo:hi] = relax(work[r, lo:hi], src, [a * CHUNK + l for l in range(CHUNK)], rows)
            return carry
        lax.fori_loop(0, count // step, body, 0)

    def own_turn(k):
        lo, hi, dl = blk, width, dlo - blk

        def rows(f, l):
            return slice(f * SUBL, l * SUBL)

        def in_play(g):
            return range(g // tiles_per_chunk * tiles_per_chunk, tiles) if g < tiles else range(0)

        def runs(ts):
            out = []
            for t in ts:
                if out and out[-1][1] == t and t - out[-1][0] < 4:
                    out[-1][1] = t + 1
                else:
                    out.append([t, t + 1])
            return out

        def expand(g, f, l, vals):
            for n in range(SUBL):
                lanes[g % 2, n, rows(f, l), :] = lane_bcast(vals, dl + g * SUBL + n)

        def relaxed(g, f, l, cur):
            acc = work[rows(f, l), lo:hi]
            for n in range(SUBL):
                acc = jnp.minimum(acc, widen(lanes[g % 2, n, rows(f, l), :], hi - lo) + jnp.broadcast_to(cur[n:n + 1, :], acc.shape))
            return acc

        def relax_tiles(g, ts, cur):
            for f, l in runs(ts):
                vals = relaxed(g, f, l, cur)
                work[rows(f, l), lo:hi] = vals
                if f in in_play(g + 1):
                    expand(g + 1, f, l, vals)

        work[rows(0, 1), lo:hi] = close_tile(work[rows(0, 1), lo:hi], dl)
        for f, l in runs(range(1, tiles)):
            expand(0, f, l, work[rows(f, l), lo:hi])
        for g in range(tiles):
            a = g // tiles_per_chunk
            cur = work[rows(g, g + 1), lo:hi]
            rest = [t for t in in_play(g) if t not in (g, g + 1)]
            if (g + 1) % tiles_per_chunk == 0:
                relax_tiles(g, [t for t in rest if t < g], cur)
                rest = [t for t in rest if t > g]
                r = slice(a * CHUNK, (a + 1) * CHUNK)
                rowp[k, a, :, 0:blk] = work[r, dlo:width]
                rowp[k, a, :, blk:dlo] = work[r, blk:dlo]
                rowp[k, a, :, dlo:width] = work[r, dlo:width]
                @pl.when((k + 1 < nrows) & (my_col == (k + 1) % ncols))
                def _():
                    nxt_copy(k, a, 1).start()
                row_copy(k, a, 0).start()
                row_copy(k, a, 2).start()
                @pl.when((k + 1 < nrows) & (my_col == (k + 1) % ncols))
                def _():
                    for d in range(2, ncols):
                        nxt_copy(k, a, d).start()
                row_copy(k, a, 1).start()
            if g + 1 < tiles:
                nxt = relaxed(g, g + 1, g + 2, cur)
                wide = jnp.concatenate([lane_bcast(nxt, dl + (g + 1) * SUBL + n) for n in range(SUBL)] + [nxt], axis=1)
                if g in in_play(g + 1):
                    expand(g + 1, g, g + 1, cur)
            relax_tiles(g, rest, cur)
            if g + 1 < tiles:
                for p in range(SUBL):
                    piv, wide = wide[:, :LANES], wide[:, LANES:]
                    wide = jnp.minimum(wide, widen(piv, wide.shape[1]) + jnp.broadcast_to(wide[p:p + 1, :], wide.shape))
                work[rows(g + 1, g + 2), lo:hi] = wide
        for a in range(1, nchunk):
            apply_rows(blk, width, dlo, k, a, a * CHUNK, CHUNK)

    def recv_row(k, a):
        fwd_copy(k, a).wait_recv()

        @pl.when(fwd_here(k))
        def _():
            fwd_copy(k, a).start()

        @pl.when(far_here(k, a))
        def _():
            far_copy(k, a).start()

    def next_turn(k):
        holder = my_col == (k + 1) % ncols
        recv_row(k, 0)
        for h in range(HALVES):
            recv_col(k, h)
        recv_diag()
        for a in range(nchunk):
            if a > 0:
                recv_row(k, a)

            @pl.when(holder)
            def _():
                rowp[k, a, :, dlo:width] = rowp[k, a, :, own_cols(k + 1)]

            @pl.when(jnp.logical_not(holder))
            def _():
                nxt_copy(k, a, 1).wait_recv()
            apply_rows(0 if a < nchunk - 1 else blk, width, 0, k, a, blk, blk)

    def relax_half(k, a, h, sections, save=False, load=False):
        r = half_rows(h)
        accs = [work[r, c] for c in sections]
        src = work[r, 0:blk]
        for n in range(CHUNK):
            if load:
                wide = spread[a * CHUNK + n, r, :]
            else:
                wide = lane_bcast(src, a * CHUNK + n)
            if save:
                spread[a * CHUNK + n, r, :] = wide
            accs = [jnp.minimum(acc, widen(wide, acc.shape[1]) + jnp.broadcast_to(rowp[k, a, n:n + 1, c], acc.shape))
                    for acc, c in zip(accs, sections)]
        for acc, c in zip(accs, sections):
            work[r, c] = acc

    def other_turn(k):
        first = slice(0, blk)
        holder = (k + 1 < nrows) & (my_col == (k + 1) % ncols)
        recv_row(k, 0)

        @pl.when(holder)
        def _():
            def body(h, carry):
                recv_col(k, h)
                for a in range(nchunk):
                    if a > 0:
                        @pl.when(h == 0)
                        def _():
                            recv_row(k, a)
                    secs = [first] if a < nchunk - 1 else []
                    relax_half(k, a, h, secs + [own_cols(k + 1)], save=True)
                send_col(k + 1, h)
                return carry
            lax.fori_loop(0, HALVES, body, 0)

            other = pl.ds(pl.multiple_of(own - (k + 1) // ncols * blk, LANES), blk)
            def rest(h, carry):
                for a in range(nchunk):
                    relax_half(k, a, h, [other], load=True)
                return carry
            lax.fori_loop(0, HALVES, rest, 0)

        @pl.when(jnp.logical_not(holder))
        def _():
            def body(h, carry):
                recv_col(k, h)
                for a in range(nchunk):
                    if a > 0:
                        @pl.when(h == 0)
                        def _():
                            recv_row(k, a)
                    relax_half(k, a, h, [slice(0 if a < nchunk - 1 else blk, dlo)])

                @pl.when((my_row == k + 2) & (my_col == my_row % ncols))
                def _():
                    send_diag(h)
                return carry
            lax.fori_loop(0, HALVES, body, 0)

    def round_body(k, carry):
        @pl.when(my_row == k)
        def _():
            @pl.when(k == 0)
            def _():
                recv_diag()
            own_turn(k)

            @pl.when((k + 1 < nrows) & (my_col == (k + 1) % ncols))
            def _():
                for h in range(HALVES):
                    send_col(k + 1, h)

        @pl.when(my_row == k + 1)
        def _():
            next_turn(k)

        @pl.when((my_row != k) & (my_row != k + 1))
        def _():
            other_turn(k)
        return carry

    lax.fori_loop(0, nrows, round_body, 0)

    store_out = pltpu.make_async_copy(work.at[:, blk:dlo], out_ref.at[0], io_sem.at[0])
    store_out.start()

    @pl.when(my_col == my_row % ncols)
    def _():
        for h in range(HALVES):
            for d in range(1, ncols):
                diag_copy(h, d).wait_send()

    def drain(k, carry):
        @pl.when((my_col == k % ncols) & (my_row != k))
        def _():
            for h in range(HALVES):
                for d in range(1, ncols):
                    col_copy(k, h, d, d - 1).wait_send()
        for a in range(nchunk):
            @pl.when(fwd_here(k))
            def _():
                fwd_copy(k, a).wait_send()

            @pl.when(far_here(k, a))
            def _():
                far_copy(k, a).wait_send()
        return carry
    lax.fori_loop(0, nrows, drain, 0)
    for a in range(nchunk):
        for n in range(nx - 1):
            row_copy(my_row, a, n).wait_send()

        @pl.when((my_row + 1 < nrows) & (my_col == (my_row + 1) % ncols))
        def _():
            for d in range(1, ncols):
                nxt_copy(my_row, a, d).wait_send()
    store_out.wait()


def solution(mesh):
    nsub = mesh.shape['sub']
    nrows = mesh.shape['row'] * nsub
    ncols = mesh.shape['col']
    dist_spec = P(('parts', 'row', 'sub'), None, 'col')

    def local_run(local):
        rows_local, blk, own = local.shape
        assert rows_local == 1
        nchunk = blk // CHUNK
        nx = nrows // nsub
        dma = pltpu.SemaphoreType.DMA
        vmem = lambda *s: pltpu.VMEM(s, jnp.float32)
        return pl.pallas_call(
            functools.partial(kernel, nrows, ncols, nsub, blk),
            out_shape=jax.ShapeDtypeStruct(local.shape, local.dtype),
            in_specs=[pl.BlockSpec(memory_space=pl.ANY)],
            out_specs=pl.BlockSpec(memory_space=pl.ANY),
            scratch_shapes=[
                vmem(blk, own + 2 * blk), vmem(blk, blk), vmem(nrows, blk, blk),
                vmem(nrows, nchunk, CHUNK, own + 2 * blk), vmem(2, SUBL, blk, LANES), vmem(blk, blk, LANES), dma((1,)),
                dma((nrows, HALVES, ncols - 1)), dma((nrows, HALVES)), dma((HALVES, ncols - 1)), dma((HALVES,)),
                dma((nchunk, nx - 1)), dma((nrows, nchunk)), dma((nrows, nchunk, 2)),
                dma((nchunk, ncols - 1)), dma((nchunk,)),
            ],
            compiler_params=pltpu.CompilerParams(collective_id=0, has_side_effects=True),
        )(local)

    return jax.shard_map(local_run, mesh=mesh, in_specs=(dist_spec,), out_specs=dist_spec, check_vma=False)
```

```python
import functools

import jax
import jax.numpy as jnp
from jax import lax
from jax.experimental import pallas as pl
from jax.experimental.pallas import tpu as pltpu
from jax.sharding import PartitionSpec as P

SUBL = 8
LANES = 128
CHUNK = 32
HALVES = 2
FULL = False


def relax(acc, src, cols, rows):
    for n, lane in enumerate(cols):
        acc = jnp.minimum(acc, jnp.broadcast_to(src[:, lane:lane + 1], acc.shape) + jnp.broadcast_to(rows(n), acc.shape))
    return acc


def lane_bcast(tile, lane):
    return jnp.broadcast_to(tile[:, lane:lane + 1], (tile.shape[0], LANES))


def widen(x, width):
    return jnp.concatenate([x] * (width // LANES), axis=1)


def kernel(nrows, ncols, nsub, blk, in_ref, out_ref, work, diag_in, colp, rowp, spread, io_sem,
           c_send, c_recv, s_send, s_recv, r_send, r_recv, f_send, n_send, n_recv):
    x = lax.axis_index('row')
    sub = lax.axis_index('sub')
    my_col = lax.axis_index('col')
    nx = nrows // nsub
    my_row = x * nsub + sub
    nchunk = blk // CHUNK
    half = blk // HALVES
    own = in_ref.shape[2]
    dlo = blk + own
    width = dlo + blk
    tiles = blk // SUBL
    tiles_per_chunk = CHUNK // SUBL

    def dev(row=None, col=None):
        out = {}
        if row is not None:
            out['row'] = row // nsub
            out['sub'] = row % nsub
        if col is not None:
            out['col'] = col
        return out

    def signal(target):
        pl.semaphore_signal(barrier, inc=1, device_id=target, device_id_type=pl.DeviceIdType.MESH)

    load_in = pltpu.make_async_copy(in_ref.at[0], work.at[:, blk:dlo], io_sem.at[0])
    load_in.start()
    barrier = pltpu.get_barrier_semaphore()
    for d in range(1, ncols):
        signal(dev(col=(my_col + d) % ncols))
    for d in range(1, nrows):
        signal(dev(row=(my_row + d) % nrows))
    for step, there in ((1, my_row + 1 < nrows), (-1, my_row > 0)):
        @pl.when(there)
        def _():
            for d in range(1, ncols):
                signal(dev(my_row + step, (my_col + d) % ncols))
    load_in.wait()
    middle = jnp.where((my_row > 0) & (my_row + 1 < nrows), 1, 0)
    pl.semaphore_wait(barrier, (2 + middle) * (ncols - 1) + nrows - 1)

    def remote(src, dst, ssem, rsem, target):
        return pltpu.make_async_remote_copy(src_ref=src, dst_ref=dst, send_sem=ssem, recv_sem=rsem,
                                            device_id=target, device_id_type=pl.DeviceIdType.MESH)

    def half_rows(h):
        return pl.ds(pl.multiple_of(h * half, half), half)

    def col_copy(k, h, d, n):
        part = colp.at[k, half_rows(h)]
        return remote(part, part, c_send.at[k, h, n], c_recv.at[k, h], dev(col=(my_col + d) % ncols))

    def diag_copy(h, d):
        part = diag_in.at[half_rows(h)]
        return remote(part, part, s_send.at[h, d - 1], s_recv.at[h], dev(col=(my_col + d) % ncols))

    def panel(k, a):
        lo = blk if a == nchunk - 1 else 0
        return rowp.at[k, a, :, lo:dlo]

    def row_copy(k, a, n):
        target = {'sub': (sub + 1) % nsub} if n == 0 else {'row': (x + (nx - 1, 1, 2)[n - 1]) % nx, 'sub': 0}
        return remote(panel(k, a), panel(k, a), r_send.at[a, n], r_recv.at[k, a], target)

    def fwd_copy(k, a):
        return remote(panel(k, a), panel(k, a), f_send.at[k, a, 0], r_recv.at[k, a], {'sub': (sub + 1) % nsub})

    def far_step(a):
        return 1 if a % 2 == 0 else nx - 1

    def far_copy(k, a):
        return remote(panel(k, a), panel(k, a), f_send.at[k, a, 1], r_recv.at[k, a], {'row': (x + far_step(a)) % nx, 'sub': 0})

    def fwd_here(k):
        return (sub == 0) & (x != k // nsub)

    def far_here(k, a):
        return (sub == 0) & (x == (k // nsub + far_step(a)) % nx) & (k + 1 < nrows)

    def nxt_copy(k, a, d):
        src = pl.ds(pl.multiple_of(blk + (k + 1) // ncols * blk, LANES), blk)
        return remote(rowp.at[k, a, :, src], rowp.at[k, a, :, dlo:width], n_send.at[a, d - 1], n_recv.at[a],
                      dev(k + 1, (my_col + d) % ncols))

    def own_cols(b):
        return pl.ds(pl.multiple_of(blk + b // ncols * blk, LANES), blk)

    def send_col(k, h):
        colp[k, half_rows(h)] = work[half_rows(h), own_cols(k)]
        for d in tuple(range(2, ncols - 1)) + (1, ncols - 1):
            col_copy(k, h, d, d - 1).start()

    def send_diag(h):
        diag_in[half_rows(h)] = work[half_rows(h), own_cols(my_row)]
        work[half_rows(h), dlo:width] = diag_in[half_rows(h)]
        for d in range(1, ncols):
            diag_copy(h, d).start()

    def recv_diag():
        @pl.when(my_col != my_row % ncols)
        def _():
            for h in range(HALVES):
                diag_copy(h, 1).wait_recv()
            work[:, dlo:width] = diag_in[...]

    def recv_col(k, h):
        @pl.when(my_col != k % ncols)
        def _():
            col_copy(k, h, 1, 0).wait_recv()
        work[half_rows(h), 0:blk] = colp[k, half_rows(h)]

    @pl.when((my_row <= 1) & (my_col == my_row % ncols))
    def _():
        for h in range(HALVES):
            send_diag(h)

    @pl.when((my_row != 0) & (my_col == 0))
    def _():
        for h in range(HALVES):
            send_col(0, h)

    def apply_rows(lo, hi, lane_lo, k, a, count, step):
        def body(it, carry):
            r = pl.ds(pl.multiple_of(it * step, step), step)
            rows = lambda n: rowp[k, a, n:n + 1, lo:hi]
            src = work[r, lane_lo:lane_lo + blk]
            work[r, lo:hi] = relax(work[r, lo:hi], src, [a * CHUNK + l for l in range(CHUNK)], rows)
            return carry
        lax.fori_loop(0, count // step, body, 0)

    def tile_rows(f, l):
        return slice(f * SUBL, l * SUBL)

    def close_chunk(k, a):
        dl = dlo - blk
        base = a * tiles_per_chunk
        vals = [work[tile_rows(base + t, base + t + 1), blk:width] for t in range(tiles_per_chunk)]
        for g in range(tiles_per_chunk):
            cols = [dl + (base + g) * SUBL + n for n in range(SUBL)]
            others = [t for t in range(tiles_per_chunk) if t != g]
            wide = jnp.concatenate([lane_bcast(vals[g], c) for c in cols] + [vals[g]], axis=1)
            spread = {t: [lane_bcast(vals[t], c) for c in cols] for t in others}
            for p in range(SUBL):
                piv, wide = wide[:, :LANES], wide[:, LANES:]
                wide = jnp.minimum(wide, widen(piv, wide.shape[1]) + jnp.broadcast_to(wide[p:p + 1, :], wide.shape))
            vals[g] = wide
            for t in others[g:] + others[:g]:
                for n in range(SUBL):
                    vals[t] = jnp.minimum(vals[t], widen(spread[t][n], own + blk) + jnp.broadcast_to(wide[n:n + 1, :], wide.shape))
        for t, v in enumerate(vals):
            r = tile_rows(t, t + 1)
            work[tile_rows(base + t, base + t + 1), blk:width] = v
            rowp[k, a, r, 0:blk] = v[:, dl:]
            rowp[k, a, r, blk:width] = v

    def send_chunk(k, a):
        sends_next = (k + 1 < nrows) & (my_col == (k + 1) % ncols)

        @pl.when(sends_next)
        def _():
            nxt_copy(k, a, 1).start()
        row_copy(k, a, 0).start()
        row_copy(k, a, 2).start()

        @pl.when(sends_next)
        def _():
            for d in range(2, ncols):
                nxt_copy(k, a, d).start()
        row_copy(k, a, 1).start()

        @pl.when(k + 1 == nrows)
        def _():
            row_copy(k, a, 3).start()

    def relax_by_chunk(a, f, l, step):
        for t in range(f, l, step):
            r = tile_rows(t, min(t + step, l))
            rows = lambda n: work[a * CHUNK + n:a * CHUNK + n + 1, blk:width]
            work[r, blk:width] = relax(work[r, blk:width], work[r, dlo:width], range(a * CHUNK, (a + 1) * CHUNK), rows)

    def spread_cols(a, f, l):
        r = tile_rows(f, l)
        src = work[r, dlo:width]
        for n in range(CHUNK):
            spread[n, r, :] = lane_bcast(src, a * CHUNK + n)

    def relax_spread(a, f, l):
        r = tile_rows(f, l)
        acc = work[r, blk:width]
        for n in range(CHUNK):
            row = work[a * CHUNK + n:a * CHUNK + n + 1, blk:width]
            acc = jnp.minimum(acc, widen(spread[n, r, :], own + blk) + jnp.broadcast_to(row, acc.shape))
        work[r, blk:width] = acc

    def own_turn(k):
        n = tiles_per_chunk

        close_chunk(k, 0)
        spread_cols(0, n, 2 * n)
        send_chunk(k, 0)
        relax_spread(0, n, 2 * n)
        close_chunk(k, 1)
        relax_by_chunk(0, 2 * n, 3 * n, n)
        spread_cols(1, 2 * n, 3 * n)
        send_chunk(k, 1)
        relax_spread(1, 2 * n, 3 * n)
        close_chunk(k, 2)
        relax_by_chunk(0, 3 * n, tiles, n)
        relax_by_chunk(1, 3 * n, tiles, n)
        spread_cols(2, 3 * n, tiles)
        send_chunk(k, 2)
        relax_spread(2, 3 * n, tiles)
        close_chunk(k, 3)
        send_chunk(k, 3)
        for a in range(1, nchunk):
            apply_rows(blk, width, dlo, k, a, a * CHUNK, CHUNK)

    def recv_row(k, a):
        fwd_copy(k, a).wait_recv()

        @pl.when(fwd_here(k))
        def _():
            fwd_copy(k, a).start()

        @pl.when(far_here(k, a))
        def _():
            far_copy(k, a).start()

    def relax_block(k, a, r, sections, save=False, load=False):
        accs = [work[r, c] for c in sections]
        src = work[r, 0:blk]
        for n in range(CHUNK):
            if load:
                wide = spread[a * CHUNK + n, r, :]
            else:
                wide = lane_bcast(src, a * CHUNK + n)
            if save:
                spread[a * CHUNK + n, r, :] = wide
            accs = [jnp.minimum(acc, widen(wide, acc.shape[1]) + jnp.broadcast_to(rowp[k, a, n:n + 1, c], acc.shape))
                    for acc, c in zip(accs, sections)]
        for acc, c in zip(accs, sections):
            work[r, c] = acc

    first = slice(0, blk)

    def rest(k, b):
        other = pl.ds(pl.multiple_of(own - b // ncols * blk, LANES), blk)
        def body(h, carry):
            for a in range(nchunk):
                relax_block(k, a, half_rows(h), [other], load=True)
            return carry
        lax.fori_loop(0, HALVES, body, 0)

    def next_turn(k):
        last = nchunk - 1

        def next_rows(a):
            holder = my_col == (k + 1) % ncols

            @pl.when(holder)
            def _():
                rowp[k, a, :, dlo:width] = rowp[k, a, :, own_cols(k + 1)]

            @pl.when(jnp.logical_not(holder))
            def _():
                nxt_copy(k, a, 1).wait_recv()

        recv_row(k, 0)

        def spread_last(r):
            src = work[r, 0:blk]
            for n in range(last * CHUNK, blk):
                spread[n, r, :] = lane_bcast(src, n)

        @pl.when(sub >= 0)
        def _():
            def body(h, carry):
                recv_col(k, h)
                for a in range(last):
                    if a > 0:
                        @pl.when(h == 0)
                        def _():
                            recv_row(k, a)
                    relax_block(k, a, half_rows(h), [slice(0, dlo)], save=True)
                spread_last(half_rows(h))
                return carry
            lax.fori_loop(0, HALVES, body, 0)
        recv_row(k, last)
        recv_diag()
        for a in range(last):
            next_rows(a)
            relax_block(k, a, slice(0, blk), [slice(dlo, width)], load=True)
        next_rows(last)

        def finish(h, carry):
            relax_block(k, last, half_rows(h), [slice(blk, width)], load=True)
            return carry
        lax.fori_loop(0, HALVES, finish, 0)

    def second_turn(k):
        sends_col = my_col == (k + 1) % ncols
        sends_diag = my_col == (k + 2) % ncols
        block = jnp.where(sends_col, k + 1, k + 2)
        recv_row(k, 0)

        def half_turn(h, sections, save):
            recv_col(k, h)
            for a in range(nchunk):
                if a > 0:
                    @pl.when(h == 0)
                    def _():
                        recv_row(k, a)
                relax_block(k, a, half_rows(h), sections(a), save=save)

        @pl.when(sends_col | sends_diag)
        def _():
            def body(h, carry):
                half_turn(h, lambda a: ([first] if a < nchunk - 1 else []) + [own_cols(block)], True)

                @pl.when(sends_col)
                def _():
                    send_col(k + 1, h)

                @pl.when(sends_diag)
                def _():
                    send_diag(h)
                return carry
            lax.fori_loop(0, HALVES, body, 0)
            rest(k, block)

        @pl.when(jnp.logical_not(sends_col | sends_diag))
        def _():
            def body(h, carry):
                half_turn(h, lambda a: [slice(0 if a < nchunk - 1 else blk, dlo)], False)
                return carry
            lax.fori_loop(0, HALVES, body, 0)

    def last_turn(k):
        for h in range(HALVES):
            recv_col(k, h)
        for a in range(nchunk):
            recv_row(k, a)
            relax_block(k, a, slice(0, blk), [slice(0 if a < nchunk - 1 else blk, dlo)])

    def other_turn(k):
        holder = (k + 1 < nrows) & (my_col == (k + 1) % ncols)
        recv_row(k, 0)

        @pl.when(holder)
        def _():
            def body(h, carry):
                recv_col(k, h)
                for a in range(nchunk):
                    if a > 0:
                        @pl.when(h == 0)
                        def _():
                            recv_row(k, a)
                    relax_block(k, a, half_rows(h), ([first] if a < nchunk - 1 else []) + [own_cols(k + 1)], save=True)
                send_col(k + 1, h)
                return carry
            lax.fori_loop(0, HALVES, body, 0)
            rest(k, k + 1)

        @pl.when(jnp.logical_not(holder))
        def _():
            def body(h, carry):
                recv_col(k, h)
                for a in range(nchunk):
                    if a > 0:
                        @pl.when(h == 0)
                        def _():
                            recv_row(k, a)
                    relax_block(k, a, half_rows(h), [slice(0 if a < nchunk - 1 else blk, dlo)])
                return carry
            lax.fori_loop(0, HALVES, body, 0)

    def round_body(k, carry):
        @pl.when(my_row == k)
        def _():
            @pl.when(k == 0)
            def _():
                recv_diag()
            own_turn(k)

            @pl.when((k + 1 < nrows) & (my_col == (k + 1) % ncols))
            def _():
                for h in range(HALVES):
                    send_col(k + 1, h)

        @pl.when(my_row == k + 1)
        def _():
            next_turn(k)

        @pl.when(my_row == k + 2)
        def _():
            second_turn(k)

        @pl.when(((my_row < k) & (k + 1 < nrows)) | (my_row > k + 2))
        def _():
            other_turn(k)

        @pl.when((my_row < k) & (k + 1 == nrows))
        def _():
            last_turn(k)
        return carry

    lax.fori_loop(0, nrows, round_body, 0)

    store_out = pltpu.make_async_copy(work.at[:, blk:dlo], out_ref.at[0], io_sem.at[0])
    store_out.start()

    @pl.when(my_col == my_row % ncols)
    def _():
        for h in range(HALVES):
            for d in range(1, ncols):
                diag_copy(h, d).wait_send()

    def drain(k, carry):
        @pl.when((my_col == k % ncols) & (my_row != k))
        def _():
            for h in range(HALVES):
                for d in range(1, ncols):
                    col_copy(k, h, d, d - 1).wait_send()
        for a in range(nchunk):
            @pl.when(fwd_here(k))
            def _():
                fwd_copy(k, a).wait_send()

            @pl.when(far_here(k, a))
            def _():
                far_copy(k, a).wait_send()
        return carry
    lax.fori_loop(0, nrows, drain, 0)
    for a in range(nchunk):
        for n in range(3):
            row_copy(my_row, a, n).wait_send()

        @pl.when(my_row + 1 == nrows)
        def _():
            row_copy(my_row, a, 3).wait_send()

        @pl.when((my_row + 1 < nrows) & (my_col == (my_row + 1) % ncols))
        def _():
            for d in range(1, ncols):
                nxt_copy(my_row, a, d).wait_send()
    store_out.wait()


def solution(mesh):
    nsub = mesh.shape['sub']
    nrows = mesh.shape['row'] * nsub
    ncols = mesh.shape['col']
    dist_spec = P(('parts', 'row', 'sub'), None, 'col')

    def local_run(local):
        rows_local, blk, own = local.shape
        assert rows_local == 1
        nchunk = blk // CHUNK
        nx = nrows // nsub
        dma = pltpu.SemaphoreType.DMA
        vmem = lambda *s: pltpu.VMEM(s, jnp.float32)
        return pl.pallas_call(
            functools.partial(kernel, nrows, ncols, nsub, blk),
            out_shape=jax.ShapeDtypeStruct(local.shape, local.dtype),
            in_specs=[pl.BlockSpec(memory_space=pl.ANY)],
            out_specs=pl.BlockSpec(memory_space=pl.ANY),
            scratch_shapes=[
                vmem(blk, own + 2 * blk), vmem(blk, blk), vmem(nrows, blk, blk),
                vmem(nrows, nchunk, CHUNK, own + 2 * blk), vmem(blk, blk, LANES), dma((1,)),
                dma((nrows, HALVES, ncols - 1)), dma((nrows, HALVES)), dma((HALVES, ncols - 1)), dma((HALVES,)),
                dma((nchunk, 4)), dma((nrows, nchunk)), dma((nrows, nchunk, 2)),
                dma((nchunk, ncols - 1)), dma((nchunk,)),
            ],
            compiler_params=pltpu.CompilerParams(collective_id=0, has_side_effects=True, vmem_limit_bytes=16 * 2**20),
        )(local)

    return jax.shard_map(local_run, mesh=mesh, in_specs=(dist_spec,), out_specs=dist_spec, check_vma=False)
```

```python
import functools

import jax
import jax.numpy as jnp
from jax import lax
from jax.experimental import pallas as pl
from jax.experimental.pallas import tpu as pltpu
from jax.sharding import PartitionSpec as P

SUBL = 8
LANES = 128
CHUNK = 32
PAIRS = CHUNK // 2
STEP = 64
HALVES = 2
FULL = False


def relax(acc, src, cols, rows):
    for n, lane in enumerate(cols):
        acc = jnp.minimum(acc, jnp.broadcast_to(src[:, lane:lane + 1], acc.shape) + jnp.broadcast_to(rows(n), acc.shape))
    return acc


def lane_bcast(tile, lane):
    return jnp.broadcast_to(tile[:, lane:lane + 1], (tile.shape[0], LANES))


def widen(x, width):
    return jnp.concatenate([x] * (width // LANES), axis=1)


def lane_id(rows):
    return lax.broadcasted_iota(jnp.int32, (rows, LANES), 1)


def pair_bcast(tile, lanes):
    return jnp.take_along_axis(tile, lanes, axis=1, mode='promise_in_bounds')


def pair_lanes(rows):
    return jnp.where(lane_id(rows) < LANES // 2, 0, PAIRS)


def pack_rows(block):
    low = lane_id(PAIRS) < LANES // 2
    turned = pltpu.roll(block, LANES // 2, 1)
    return jnp.where(low, block[:PAIRS], turned[PAIRS:]), jnp.where(low, turned[:PAIRS], block[PAIRS:])


def kernel(nrows, ncols, nsub, blk, in_ref, out_ref, work, diag_in, colp, rowp, spread, io_sem,
           c_send, c_recv, s_send, s_recv, r_send, r_recv, f_send, n_send, n_recv):
    x = lax.axis_index('row')
    sub = lax.axis_index('sub')
    my_col = lax.axis_index('col')
    nx = nrows // nsub
    my_row = x * nsub + sub
    nchunk = blk // CHUNK
    half = blk // HALVES
    own = in_ref.shape[2]
    dlo = blk + own
    width = dlo + blk
    tiles = blk // SUBL
    tiles_per_chunk = CHUNK // SUBL

    def dev(row=None, col=None):
        out = {}
        if row is not None:
            out['row'] = row // nsub
            out['sub'] = row % nsub
        if col is not None:
            out['col'] = col
        return out

    def signal(target):
        pl.semaphore_signal(barrier, inc=1, device_id=target, device_id_type=pl.DeviceIdType.MESH)

    load_in = pltpu.make_async_copy(in_ref.at[0], work.at[:, blk:dlo], io_sem.at[0])
    load_in.start()
    barrier = pltpu.get_barrier_semaphore()
    for d in range(1, ncols):
        signal(dev(col=(my_col + d) % ncols))
    for d in range(1, nrows):
        signal(dev(row=(my_row + d) % nrows))
    for step, there in ((1, my_row + 1 < nrows), (-1, my_row > 0)):
        @pl.when(there)
        def _():
            for d in range(1, ncols):
                signal(dev(my_row + step, (my_col + d) % ncols))
    load_in.wait()
    middle = jnp.where((my_row > 0) & (my_row + 1 < nrows), 1, 0)
    pl.semaphore_wait(barrier, (2 + middle) * (ncols - 1) + nrows - 1)

    def remote(src, dst, ssem, rsem, target):
        return pltpu.make_async_remote_copy(src_ref=src, dst_ref=dst, send_sem=ssem, recv_sem=rsem,
                                            device_id=target, device_id_type=pl.DeviceIdType.MESH)

    def half_rows(h):
        return pl.ds(pl.multiple_of(h * half, half), half)

    def col_copy(k, h, d, n):
        part = colp.at[k, half_rows(h)]
        return remote(part, part, c_send.at[k, h, n], c_recv.at[k, h], dev(col=(my_col + d) % ncols))

    def diag_copy(h, d):
        part = diag_in.at[half_rows(h)]
        return remote(part, part, s_send.at[h, d - 1], s_recv.at[h], dev(col=(my_col + d) % ncols))

    def panel(k, a):
        lo = blk if a == nchunk - 1 else 0
        return rowp.at[k, a, :, lo:dlo]

    def row_copy(k, a, n):
        target = {'sub': (sub + 1) % nsub} if n == 0 else {'row': (x + (nx - 1, 1, 2)[n - 1]) % nx, 'sub': 0}
        return remote(panel(k, a), panel(k, a), r_send.at[a, n], r_recv.at[k, a], target)

    def fwd_copy(k, a):
        return remote(panel(k, a), panel(k, a), f_send.at[k, a, 0], r_recv.at[k, a], {'sub': (sub + 1) % nsub})

    def far_step(a):
        return 1 if a % 2 == 0 else nx - 1

    def far_copy(k, a):
        return remote(panel(k, a), panel(k, a), f_send.at[k, a, 1], r_recv.at[k, a], {'row': (x + far_step(a)) % nx, 'sub': 0})

    def fwd_here(k):
        return (sub == 0) & (x != k // nsub)

    def far_here(k, a):
        return (sub == 0) & (x == (k // nsub + far_step(a)) % nx) & (k + 1 < nrows)

    def nxt_copy(k, a, d):
        src = pl.ds(pl.multiple_of(blk + (k + 1) // ncols * blk, LANES), blk)
        return remote(rowp.at[k, a, :, src], rowp.at[k, a, :, dlo:width], n_send.at[a, d - 1], n_recv.at[a],
                      dev(k + 1, (my_col + d) % ncols))

    def own_cols(b):
        return pl.ds(pl.multiple_of(blk + b // ncols * blk, LANES), blk)

    def send_col(k, h):
        colp[k, half_rows(h)] = work[half_rows(h), own_cols(k)]
        for d in tuple(range(2, ncols - 1)) + (1, ncols - 1):
            col_copy(k, h, d, d - 1).start()

    def send_diag(h):
        diag_in[half_rows(h)] = work[half_rows(h), own_cols(my_row)]
        work[half_rows(h), dlo:width] = diag_in[half_rows(h)]
        for d in range(1, ncols):
            diag_copy(h, d).start()

    def recv_diag():
        @pl.when(my_col != my_row % ncols)
        def _():
            for h in range(HALVES):
                diag_copy(h, 1).wait_recv()
            work[:, dlo:width] = diag_in[...]

    def recv_col(k, h):
        @pl.when(my_col != k % ncols)
        def _():
            col_copy(k, h, 1, 0).wait_recv()
        work[half_rows(h), 0:blk] = colp[k, half_rows(h)]

    @pl.when((my_row <= 1) & (my_col == my_row % ncols))
    def _():
        for h in range(HALVES):
            send_diag(h)

    @pl.when((my_row != 0) & (my_col == 0))
    def _():
        for h in range(HALVES):
            send_col(0, h)

    def tile_rows(f, l):
        return slice(f * SUBL, l * SUBL)

    def close_chunk(k, a):
        dl = dlo - blk
        base = a * tiles_per_chunk
        vals = [work[tile_rows(base + t, base + t + 1), blk:width] for t in range(tiles_per_chunk)]
        for g in range(tiles_per_chunk):
            cols = [dl + (base + g) * SUBL + n for n in range(SUBL)]
            others = [t for t in range(tiles_per_chunk) if t != g]
            wide = jnp.concatenate([lane_bcast(vals[g], c) for c in cols] + [vals[g]], axis=1)
            spread = {t: [lane_bcast(vals[t], c) for c in cols] for t in others}
            for p in range(SUBL):
                piv, wide = wide[:, :LANES], wide[:, LANES:]
                wide = jnp.minimum(wide, widen(piv, wide.shape[1]) + jnp.broadcast_to(wide[p:p + 1, :], wide.shape))
            vals[g] = wide
            for t in others[g:] + others[:g]:
                for n in range(SUBL):
                    vals[t] = jnp.minimum(vals[t], widen(spread[t][n], own + blk) + jnp.broadcast_to(wide[n:n + 1, :], wide.shape))
        for t, v in enumerate(vals):
            work[tile_rows(base + t, base + t + 1), blk:width] = v
        for c in range(0, own + blk, LANES):
            packed = pack_rows(jnp.concatenate([v[:, c:c + LANES] for v in vals], axis=0))
            for n, v in enumerate(packed):
                r = slice(n * PAIRS, (n + 1) * PAIRS)
                rowp[k, a, r, blk + c:blk + c + LANES] = v
                if c == dl:
                    rowp[k, a, r, 0:blk] = v

    def send_chunk(k, a):
        sends_next = (k + 1 < nrows) & (my_col == (k + 1) % ncols)

        @pl.when(sends_next)
        def _():
            nxt_copy(k, a, 1).start()
        row_copy(k, a, 0).start()
        row_copy(k, a, 2).start()

        @pl.when(sends_next)
        def _():
            for d in range(2, ncols):
                nxt_copy(k, a, d).start()
        row_copy(k, a, 1).start()

        @pl.when(k + 1 == nrows)
        def _():
            row_copy(k, a, 3).start()

    def relax_by_chunk(a, f, l, step):
        for t in range(f, l, step):
            r = tile_rows(t, min(t + step, l))
            rows = lambda n: work[a * CHUNK + n:a * CHUNK + n + 1, blk:width]
            work[r, blk:width] = relax(work[r, blk:width], work[r, dlo:width], range(a * CHUNK, (a + 1) * CHUNK), rows)

    def spread_cols(a, f, l):
        r = tile_rows(f, l)
        src = work[r, dlo:width]
        for n in range(CHUNK):
            spread[n, r, :] = lane_bcast(src, a * CHUNK + n)

    def relax_spread(a, f, l):
        r = tile_rows(f, l)
        acc = work[r, blk:width]
        for n in range(CHUNK):
            row = work[a * CHUNK + n:a * CHUNK + n + 1, blk:width]
            acc = jnp.minimum(acc, widen(spread[n, r, :], own + blk) + jnp.broadcast_to(row, acc.shape))
        work[r, blk:width] = acc

    def own_turn(k):
        n = tiles_per_chunk

        close_chunk(k, 0)
        spread_cols(0, n, 2 * n)
        send_chunk(k, 0)
        relax_spread(0, n, 2 * n)
        close_chunk(k, 1)
        relax_by_chunk(0, 2 * n, 3 * n, n)
        spread_cols(1, 2 * n, 3 * n)
        send_chunk(k, 1)
        relax_spread(1, 2 * n, 3 * n)
        close_chunk(k, 2)
        relax_by_chunk(0, 3 * n, tiles, n)
        relax_by_chunk(1, 3 * n, tiles, n)
        spread_cols(2, 3 * n, tiles)
        send_chunk(k, 2)
        relax_spread(2, 3 * n, tiles)
        close_chunk(k, 3)
        send_chunk(k, 3)
        for a in range(1, nchunk):
            def body(it, carry):
                r = pl.ds(pl.multiple_of(it * CHUNK, CHUNK), CHUNK)
                rows = lambda n: work[a * CHUNK + n:a * CHUNK + n + 1, blk:width]
                work[r, blk:width] = relax(work[r, blk:width], work[r, dlo:width], range(a * CHUNK, (a + 1) * CHUNK), rows)
                return carry
            lax.fori_loop(0, a, body, 0)

    def recv_row(k, a):
        fwd_copy(k, a).wait_recv()

        @pl.when(fwd_here(k))
        def _():
            fwd_copy(k, a).start()

        @pl.when(far_here(k, a))
        def _():
            far_copy(k, a).start()

    def relax_block(k, a, start, count, sections, save=False, load=False):
        low = lane_id(STEP) < LANES // 2
        pairs = pair_lanes(STEP)
        sizes = [c.size if isinstance(c, pl.Slice) else c.stop - c.start for c in sections]
        for i in range(count // STEP):
            r = pl.ds(pl.multiple_of(start + i * STEP, STEP), STEP)
            src = None if load else work[r, 0:blk]
            accs = [None] * len(sections)
            for n in range(PAIRS):
                if load:
                    wide = spread[a * PAIRS + n, r, :]
                else:
                    wide = pair_bcast(src, pairs + (a * CHUNK + n))
                if save:
                    spread[a * PAIRS + n, r, :] = wide
                for c, (cols, size) in enumerate(zip(sections, sizes)):
                    reps = widen(wide, size)
                    new = [reps + jnp.broadcast_to(rowp[k, a, m:m + 1, cols], reps.shape) for m in (n, n + PAIRS)]
                    accs[c] = new if n == 0 else [jnp.minimum(x, y) for x, y in zip(accs[c], new)]
            for (lower, upper), cols in zip(accs, sections):
                parts = []
                for b in range(0, lower.shape[1], LANES):
                    x, y = lower[:, b:b + LANES], upper[:, b:b + LANES]
                    parts.append(jnp.minimum(jnp.where(low, x, y), pltpu.roll(jnp.where(low, y, x), LANES // 2, 1)))
                work[r, cols] = jnp.minimum(work[r, cols], jnp.concatenate(parts, axis=1))


    first = slice(0, blk)

    def rest(k, b):
        other = pl.ds(pl.multiple_of(own - b // ncols * blk, LANES), blk)
        def body(h, carry):
            for a in range(nchunk):
                relax_block(k, a, h * half, half, [other], load=True)
            return carry
        lax.fori_loop(0, HALVES, body, 0)

    def next_turn(k):
        last = nchunk - 1

        def next_rows(a):
            holder = my_col == (k + 1) % ncols

            @pl.when(holder)
            def _():
                rowp[k, a, :, dlo:width] = rowp[k, a, :, own_cols(k + 1)]

            @pl.when(jnp.logical_not(holder))
            def _():
                nxt_copy(k, a, 1).wait_recv()

        recv_row(k, 0)

        def spread_last(h):
            src = work[half_rows(h), 0:blk]
            pairs = pair_lanes(half)
            for n in range(PAIRS):
                spread[last * PAIRS + n, half_rows(h), :] = pair_bcast(src, pairs + (last * CHUNK + n))

        @pl.when(sub >= 0)
        def _():
            def body(h, carry):
                recv_col(k, h)
                for a in range(last):
                    if a > 0:
                        @pl.when(h == 0)
                        def _():
                            recv_row(k, a)
                    relax_block(k, a, h * half, half, [slice(0, dlo)], save=True)
                spread_last(h)
                return carry
            lax.fori_loop(0, HALVES, body, 0)
        recv_row(k, last)
        recv_diag()
        for a in range(last):
            next_rows(a)
            relax_block(k, a, 0, blk, [slice(dlo, width)], load=True)
        next_rows(last)

        def finish(h, carry):
            relax_block(k, last, h * half, half, [slice(blk, width)], load=True)
            return carry
        lax.fori_loop(0, HALVES, finish, 0)

    def second_turn(k):
        sends_col = my_col == (k + 1) % ncols
        sends_diag = my_col == (k + 2) % ncols
        block = jnp.where(sends_col, k + 1, k + 2)
        recv_row(k, 0)

        def half_turn(h, sections, save):
            recv_col(k, h)
            for a in range(nchunk):
                if a > 0:
                    @pl.when(h == 0)
                    def _():
                        recv_row(k, a)
                relax_block(k, a, h * half, half, sections(a), save=save)

        @pl.when(sends_col | sends_diag)
        def _():
            def body(h, carry):
                half_turn(h, lambda a: ([first] if a < nchunk - 1 else []) + [own_cols(block)], True)

                @pl.when(sends_col)
                def _():
                    send_col(k + 1, h)

                @pl.when(sends_diag)
                def _():
                    send_diag(h)
                return carry
            lax.fori_loop(0, HALVES, body, 0)
            rest(k, block)

        @pl.when(jnp.logical_not(sends_col | sends_diag))
        def _():
            def body(h, carry):
                half_turn(h, lambda a: [slice(0 if a < nchunk - 1 else blk, dlo)], False)
                return carry
            lax.fori_loop(0, HALVES, body, 0)

    def last_turn(k):
        for h in range(HALVES):
            recv_col(k, h)
        for a in range(nchunk):
            recv_row(k, a)
            relax_block(k, a, 0, blk, [slice(0 if a < nchunk - 1 else blk, dlo)])

    def other_turn(k):
        holder = (k + 1 < nrows) & (my_col == (k + 1) % ncols)
        recv_row(k, 0)

        @pl.when(holder)
        def _():
            def body(h, carry):
                recv_col(k, h)
                for a in range(nchunk):
                    if a > 0:
                        @pl.when(h == 0)
                        def _():
                            recv_row(k, a)
                    relax_block(k, a, h * half, half, ([first] if a < nchunk - 1 else []) + [own_cols(k + 1)], save=True)
                send_col(k + 1, h)
                return carry
            lax.fori_loop(0, HALVES, body, 0)
            rest(k, k + 1)

        @pl.when(jnp.logical_not(holder))
        def _():
            def body(h, carry):
                recv_col(k, h)
                for a in range(nchunk):
                    if a > 0:
                        @pl.when(h == 0)
                        def _():
                            recv_row(k, a)
                    relax_block(k, a, h * half, half, [slice(0 if a < nchunk - 1 else blk, dlo)])
                return carry
            lax.fori_loop(0, HALVES, body, 0)

    def round_body(k, carry):
        @pl.when(my_row == k)
        def _():
            @pl.when(k == 0)
            def _():
                recv_diag()
            own_turn(k)

            @pl.when((k + 1 < nrows) & (my_col == (k + 1) % ncols))
            def _():
                for h in range(HALVES):
                    send_col(k + 1, h)

        @pl.when(my_row == k + 1)
        def _():
            next_turn(k)

        @pl.when(my_row == k + 2)
        def _():
            second_turn(k)

        @pl.when(((my_row < k) & (k + 1 < nrows)) | (my_row > k + 2))
        def _():
            other_turn(k)

        @pl.when((my_row < k) & (k + 1 == nrows))
        def _():
            last_turn(k)
        return carry

    lax.fori_loop(0, nrows, round_body, 0)

    store_out = pltpu.make_async_copy(work.at[:, blk:dlo], out_ref.at[0], io_sem.at[0])
    store_out.start()

    @pl.when(my_col == my_row % ncols)
    def _():
        for h in range(HALVES):
            for d in range(1, ncols):
                diag_copy(h, d).wait_send()

    def drain(k, carry):
        @pl.when((my_col == k % ncols) & (my_row != k))
        def _():
            for h in range(HALVES):
                for d in range(1, ncols):
                    col_copy(k, h, d, d - 1).wait_send()
        for a in range(nchunk):
            @pl.when(fwd_here(k))
            def _():
                fwd_copy(k, a).wait_send()

            @pl.when(far_here(k, a))
            def _():
                far_copy(k, a).wait_send()
        return carry
    lax.fori_loop(0, nrows, drain, 0)
    for a in range(nchunk):
        for n in range(3):
            row_copy(my_row, a, n).wait_send()

        @pl.when(my_row + 1 == nrows)
        def _():
            row_copy(my_row, a, 3).wait_send()

        @pl.when((my_row + 1 < nrows) & (my_col == (my_row + 1) % ncols))
        def _():
            for d in range(1, ncols):
                nxt_copy(my_row, a, d).wait_send()
    store_out.wait()


def solution(mesh):
    nsub = mesh.shape['sub']
    nrows = mesh.shape['row'] * nsub
    ncols = mesh.shape['col']
    dist_spec = P(('parts', 'row', 'sub'), None, 'col')

    def local_run(local):
        rows_local, blk, own = local.shape
        assert rows_local == 1
        nchunk = blk // CHUNK
        nx = nrows // nsub
        dma = pltpu.SemaphoreType.DMA
        vmem = lambda *s: pltpu.VMEM(s, jnp.float32)
        return pl.pallas_call(
            functools.partial(kernel, nrows, ncols, nsub, blk),
            out_shape=jax.ShapeDtypeStruct(local.shape, local.dtype),
            in_specs=[pl.BlockSpec(memory_space=pl.ANY)],
            out_specs=pl.BlockSpec(memory_space=pl.ANY),
            scratch_shapes=[
                vmem(blk, own + 2 * blk), vmem(blk, blk), vmem(nrows, blk, blk),
                vmem(nrows, nchunk, CHUNK, own + 2 * blk), vmem(blk, blk, LANES), dma((1,)),
                dma((nrows, HALVES, ncols - 1)), dma((nrows, HALVES)), dma((HALVES, ncols - 1)), dma((HALVES,)),
                dma((nchunk, 4)), dma((nrows, nchunk)), dma((nrows, nchunk, 2)),
                dma((nchunk, ncols - 1)), dma((nchunk,)),
            ],
            compiler_params=pltpu.CompilerParams(collective_id=0, has_side_effects=True, vmem_limit_bytes=16 * 2**20),
        )(local)

    return jax.shard_map(local_run, mesh=mesh, in_specs=(dist_spec,), out_specs=dist_spec, check_vma=False)
```

```python
import functools

import jax
import jax.numpy as jnp
from jax import lax
from jax.experimental import pallas as pl
from jax.experimental.pallas import tpu as pltpu
from jax.sharding import PartitionSpec as P

SUBL = 8
LANES = 128
CHUNK = 32
PAIRS = CHUNK // 2
STEP = 64
HALVES = 2
FULL = False


def relax(acc, src, cols, rows):
    for n, lane in enumerate(cols):
        acc = jnp.minimum(acc, jnp.broadcast_to(src[:, lane:lane + 1], acc.shape) + jnp.broadcast_to(rows(n), acc.shape))
    return acc


def lane_bcast(tile, lane):
    return jnp.broadcast_to(tile[:, lane:lane + 1], (tile.shape[0], LANES))


def widen(x, width):
    return jnp.concatenate([x] * (width // LANES), axis=1)


def lane_id(rows):
    return lax.broadcasted_iota(jnp.int32, (rows, LANES), 1)


def pair_bcast(tile, lanes):
    return jnp.take_along_axis(tile, lanes, axis=1, mode='promise_in_bounds')


def pair_lanes(rows):
    return jnp.where(lane_id(rows) < LANES // 2, 0, PAIRS)


def pack_rows(block):
    low = lane_id(PAIRS) < LANES // 2
    turned = pltpu.roll(block, LANES // 2, 1)
    return jnp.where(low, block[:PAIRS], turned[PAIRS:]), jnp.where(low, turned[:PAIRS], block[PAIRS:])


def kernel(nrows, ncols, nsub, blk, in_ref, out_ref, work, diag_in, colp, rowp, spread, io_sem,
           c_send, c_recv, s_send, s_recv, r_send, r_recv, f_send, n_send, n_recv):
    x = lax.axis_index('row')
    sub = lax.axis_index('sub')
    my_col = lax.axis_index('col')
    nx = nrows // nsub
    my_row = x * nsub + sub
    nchunk = blk // CHUNK
    half = blk // HALVES
    own = in_ref.shape[2]
    dlo = blk + own
    width = dlo + blk
    tiles = blk // SUBL
    tiles_per_chunk = CHUNK // SUBL

    def dev(row=None, col=None):
        out = {}
        if row is not None:
            out['row'] = row // nsub
            out['sub'] = row % nsub
        if col is not None:
            out['col'] = col
        return out

    def signal(target):
        pl.semaphore_signal(barrier, inc=1, device_id=target, device_id_type=pl.DeviceIdType.MESH)

    load_in = pltpu.make_async_copy(in_ref.at[0], work.at[:, blk:dlo], io_sem.at[0])
    load_in.start()
    barrier = pltpu.get_barrier_semaphore()
    for d in range(1, ncols):
        signal(dev(col=(my_col + d) % ncols))
    for d in range(1, nrows):
        signal(dev(row=(my_row + d) % nrows))
    for step, there in ((1, my_row + 1 < nrows), (-1, my_row > 0)):
        @pl.when(there)
        def _():
            for d in range(1, ncols):
                signal(dev(my_row + step, (my_col + d) % ncols))
    load_in.wait()
    middle = jnp.where((my_row > 0) & (my_row + 1 < nrows), 1, 0)
    pl.semaphore_wait(barrier, (2 + middle) * (ncols - 1) + nrows - 1)

    def remote(src, dst, ssem, rsem, target):
        return pltpu.make_async_remote_copy(src_ref=src, dst_ref=dst, send_sem=ssem, recv_sem=rsem,
                                            device_id=target, device_id_type=pl.DeviceIdType.MESH)

    def half_rows(h):
        return pl.ds(pl.multiple_of(h * half, half), half)

    def col_copy(k, h, d, n):
        part = colp.at[k, half_rows(h)]
        return remote(part, part, c_send.at[k, h, n], c_recv.at[k, h], dev(col=(my_col + d) % ncols))

    def diag_copy(h, d):
        part = diag_in.at[half_rows(h)]
        return remote(part, part, s_send.at[h, d - 1], s_recv.at[h], dev(col=(my_col + d) % ncols))

    def panel(k, a):
        lo = blk if a == nchunk - 1 else 0
        return rowp.at[k, a, :, lo:dlo]

    def row_copy(k, a, n):
        target = {'sub': (sub + 1) % nsub} if n == 0 else {'row': (x + (nx - 1, 1, 2)[n - 1]) % nx, 'sub': 0}
        return remote(panel(k, a), panel(k, a), r_send.at[a, n], r_recv.at[k, a], target)

    def fwd_copy(k, a):
        return remote(panel(k, a), panel(k, a), f_send.at[k, a, 0], r_recv.at[k, a], {'sub': (sub + 1) % nsub})

    def far_step(a):
        return 1 if a % 2 == 0 else nx - 1

    def far_copy(k, a):
        return remote(panel(k, a), panel(k, a), f_send.at[k, a, 1], r_recv.at[k, a], {'row': (x + far_step(a)) % nx, 'sub': 0})

    def fwd_here(k):
        return (sub == 0) & (x != k // nsub)

    def far_here(k, a):
        return (sub == 0) & (x == (k // nsub + far_step(a)) % nx) & (k + 1 < nrows)

    def nxt_copy(k, a, d):
        src = pl.ds(pl.multiple_of(blk + (k + 1) // ncols * blk, LANES), blk)
        return remote(rowp.at[k, a, :, src], rowp.at[k, a, :, dlo:width], n_send.at[a, d - 1], n_recv.at[a],
                      dev(k + 1, (my_col + d) % ncols))

    def own_cols(b):
        return pl.ds(pl.multiple_of(blk + b // ncols * blk, LANES), blk)

    def send_col(k, h):
        colp[k, half_rows(h)] = work[half_rows(h), own_cols(k)]
        for d in tuple(range(2, ncols - 1)) + (1, ncols - 1):
            col_copy(k, h, d, d - 1).start()

    def send_diag(h):
        diag_in[half_rows(h)] = work[half_rows(h), own_cols(my_row)]
        work[half_rows(h), dlo:width] = diag_in[half_rows(h)]
        for d in range(1, ncols):
            diag_copy(h, d).start()

    def recv_diag():
        @pl.when(my_col != my_row % ncols)
        def _():
            for h in range(HALVES):
                diag_copy(h, 1).wait_recv()
            work[:, dlo:width] = diag_in[...]

    def recv_col(k, h):
        @pl.when(my_col != k % ncols)
        def _():
            col_copy(k, h, 1, 0).wait_recv()
        work[half_rows(h), 0:blk] = colp[k, half_rows(h)]

    @pl.when((my_row <= 1) & (my_col == my_row % ncols))
    def _():
        for h in range(HALVES):
            send_diag(h)

    @pl.when((my_row != 0) & (my_col == 0))
    def _():
        for h in range(HALVES):
            send_col(0, h)

    def tile_rows(f, l):
        return slice(f * SUBL, l * SUBL)

    def close_chunk(k, a):
        dl = dlo - blk
        base = a * tiles_per_chunk
        vals = [work[tile_rows(base + t, base + t + 1), blk:width] for t in range(tiles_per_chunk)]
        for g in range(tiles_per_chunk):
            cols = [dl + (base + g) * SUBL + n for n in range(SUBL)]
            others = [t for t in range(tiles_per_chunk) if t != g]
            wide = jnp.concatenate([lane_bcast(vals[g], c) for c in cols] + [vals[g]], axis=1)
            spread = {t: [lane_bcast(vals[t], c) for c in cols] for t in others}
            for p in range(SUBL):
                piv, wide = wide[:, :LANES], wide[:, LANES:]
                wide = jnp.minimum(wide, widen(piv, wide.shape[1]) + jnp.broadcast_to(wide[p:p + 1, :], wide.shape))
            vals[g] = wide
            for t in others[g:] + others[:g]:
                for n in range(SUBL):
                    vals[t] = jnp.minimum(vals[t], widen(spread[t][n], own + blk) + jnp.broadcast_to(wide[n:n + 1, :], wide.shape))
        for t, v in enumerate(vals):
            work[tile_rows(base + t, base + t + 1), blk:width] = v
        for c in range(0, own + blk, LANES):
            packed = pack_rows(jnp.concatenate([v[:, c:c + LANES] for v in vals], axis=0))
            for n, v in enumerate(packed):
                r = slice(n * PAIRS, (n + 1) * PAIRS)
                rowp[k, a, r, blk + c:blk + c + LANES] = v
                if c == dl:
                    rowp[k, a, r, 0:blk] = v

    def send_chunk(k, a):
        sends_next = (k + 1 < nrows) & (my_col == (k + 1) % ncols)

        @pl.when(sends_next)
        def _():
            nxt_copy(k, a, 1).start()
        row_copy(k, a, 0).start()
        row_copy(k, a, 2).start()

        @pl.when(sends_next)
        def _():
            for d in range(2, ncols):
                nxt_copy(k, a, d).start()
        row_copy(k, a, 1).start()

        @pl.when(k + 1 == nrows)
        def _():
            row_copy(k, a, 3).start()

    def relax_by_chunk(a, f, l, step):
        for t in range(f, l, step):
            r = tile_rows(t, min(t + step, l))
            rows = lambda n: work[a * CHUNK + n:a * CHUNK + n + 1, blk:width]
            work[r, blk:width] = relax(work[r, blk:width], work[r, dlo:width], range(a * CHUNK, (a + 1) * CHUNK), rows)

    def spread_cols(a, f, l):
        r = tile_rows(f, l)
        src = work[r, dlo:width]
        for n in range(CHUNK):
            spread[n, r, :] = lane_bcast(src, a * CHUNK + n)

    def relax_spread(a, f, l):
        r = tile_rows(f, l)
        acc = work[r, blk:width]
        for n in range(CHUNK):
            row = work[a * CHUNK + n:a * CHUNK + n + 1, blk:width]
            acc = jnp.minimum(acc, widen(spread[n, r, :], own + blk) + jnp.broadcast_to(row, acc.shape))
        work[r, blk:width] = acc

    def own_turn(k):
        n = tiles_per_chunk

        close_chunk(k, 0)
        spread_cols(0, n, 2 * n)
        send_chunk(k, 0)
        relax_spread(0, n, 2 * n)
        close_chunk(k, 1)
        relax_by_chunk(0, 2 * n, 3 * n, n)
        spread_cols(1, 2 * n, 3 * n)
        send_chunk(k, 1)
        relax_spread(1, 2 * n, 3 * n)
        close_chunk(k, 2)
        relax_by_chunk(0, 3 * n, tiles, n)
        relax_by_chunk(1, 3 * n, tiles, n)
        spread_cols(2, 3 * n, tiles)
        send_chunk(k, 2)
        relax_spread(2, 3 * n, tiles)
        close_chunk(k, 3)
        send_chunk(k, 3)
        for a in range(1, nchunk):
            def body(it, carry):
                r = pl.ds(pl.multiple_of(it * CHUNK, CHUNK), CHUNK)
                rows = lambda n: work[a * CHUNK + n:a * CHUNK + n + 1, blk:width]
                work[r, blk:width] = relax(work[r, blk:width], work[r, dlo:width], range(a * CHUNK, (a + 1) * CHUNK), rows)
                return carry
            lax.fori_loop(0, a, body, 0)

    def recv_row(k, a):
        fwd_copy(k, a).wait_recv()

        @pl.when(fwd_here(k))
        def _():
            fwd_copy(k, a).start()

        @pl.when(far_here(k, a))
        def _():
            far_copy(k, a).start()

    def relax_block(k, a, start, count, sections, save=False, load=False):
        low = lane_id(STEP) < LANES // 2
        pairs = pair_lanes(STEP)
        sizes = [c.size if isinstance(c, pl.Slice) else c.stop - c.start for c in sections]
        for i in range(count // STEP):
            r = pl.ds(pl.multiple_of(start + i * STEP, STEP), STEP)
            src = None if load else work[r, 0:blk]
            accs = [None] * len(sections)
            for n in range(PAIRS):
                if load:
                    wide = spread[a * PAIRS + n, r, :]
                else:
                    wide = pair_bcast(src, pairs + (a * CHUNK + n))
                if save:
                    spread[a * PAIRS + n, r, :] = wide
                for c, (cols, size) in enumerate(zip(sections, sizes)):
                    reps = widen(wide, size)
                    new = [reps + jnp.broadcast_to(rowp[k, a, m:m + 1, cols], reps.shape) for m in (n, n + PAIRS)]
                    accs[c] = new if n == 0 else [jnp.minimum(x, y) for x, y in zip(accs[c], new)]
            for (lower, upper), cols in zip(accs, sections):
                parts = []
                for b in range(0, lower.shape[1], LANES):
                    x, y = lower[:, b:b + LANES], upper[:, b:b + LANES]
                    parts.append(jnp.minimum(jnp.where(low, x, y), pltpu.roll(jnp.where(low, y, x), LANES // 2, 1)))
                work[r, cols] = jnp.minimum(work[r, cols], jnp.concatenate(parts, axis=1))


    first = slice(0, blk)

    def rest(k, b):
        other = pl.ds(pl.multiple_of(own - b // ncols * blk, LANES), blk)
        def body(h, carry):
            for a in range(nchunk):
                relax_block(k, a, h * half, half, [other], load=True)
            return carry
        lax.fori_loop(0, HALVES, body, 0)

    def next_turn(k):
        last = nchunk - 1

        def next_rows(a):
            holder = my_col == (k + 1) % ncols

            @pl.when(holder)
            def _():
                rowp[k, a, :, dlo:width] = rowp[k, a, :, own_cols(k + 1)]

            @pl.when(jnp.logical_not(holder))
            def _():
                nxt_copy(k, a, 1).wait_recv()

        recv_row(k, 0)

        def spread_last(h):
            src = work[half_rows(h), 0:blk]
            pairs = pair_lanes(half)
            for n in range(PAIRS):
                spread[last * PAIRS + n, half_rows(h), :] = pair_bcast(src, pairs + (last * CHUNK + n))

        @pl.when(sub >= 0)
        def _():
            def body(h, carry):
                recv_col(k, h)
                for a in range(last):
                    if a > 0:
                        @pl.when(h == 0)
                        def _():
                            recv_row(k, a)
                    relax_block(k, a, h * half, half, [slice(0, dlo)], save=True)
                spread_last(h)

                @pl.when((h == 0) & (sub == 0))
                def _():
                    recv_row(k, last)
                return carry
            lax.fori_loop(0, HALVES, body, 0)

        @pl.when(sub > 0)
        def _():
            recv_row(k, last)
        recv_diag()
        for a in range(last):
            next_rows(a)
            relax_block(k, a, 0, blk, [slice(dlo, width)], load=True)
        next_rows(last)

        def finish(h, carry):
            relax_block(k, last, h * half, half, [slice(blk, width)], load=True)
            return carry
        lax.fori_loop(0, HALVES, finish, 0)

    def second_turn(k):
        sends_col = my_col == (k + 1) % ncols
        sends_diag = my_col == (k + 2) % ncols
        block = jnp.where(sends_col, k + 1, k + 2)
        recv_row(k, 0)

        def half_turn(h, sections, save):
            recv_col(k, h)
            for a in range(nchunk):
                if a > 0:
                    @pl.when(h == 0)
                    def _():
                        recv_row(k, a)
                relax_block(k, a, h * half, half, sections(a), save=save)

        @pl.when(sends_col | sends_diag)
        def _():
            def body(h, carry):
                half_turn(h, lambda a: ([first] if a < nchunk - 1 else []) + [own_cols(block)], True)

                @pl.when(sends_col)
                def _():
                    send_col(k + 1, h)

                @pl.when(sends_diag)
                def _():
                    send_diag(h)
                return carry
            lax.fori_loop(0, HALVES, body, 0)
            rest(k, block)

        @pl.when(jnp.logical_not(sends_col | sends_diag))
        def _():
            def body(h, carry):
                half_turn(h, lambda a: [slice(0 if a < nchunk - 1 else blk, dlo)], False)
                return carry
            lax.fori_loop(0, HALVES, body, 0)

    def store_half(h):
        return pltpu.make_async_copy(work.at[half_rows(h), blk:dlo], out_ref.at[0, half_rows(h)], io_sem.at[h])

    def last_turn(k):
        recv_row(k, 0)

        def body(h, carry):
            recv_col(k, h)
            for a in range(nchunk):
                if a > 0:
                    @pl.when(h == 0)
                    def _():
                        recv_row(k, a)
                relax_block(k, a, h * half, half, [slice(0 if a < nchunk - 1 else blk, dlo)])
            store_half(h).start()
            return carry
        lax.fori_loop(0, HALVES, body, 0)

    def other_turn(k):
        holder = (k + 1 < nrows) & (my_col == (k + 1) % ncols)
        recv_row(k, 0)

        @pl.when(holder)
        def _():
            def body(h, carry):
                recv_col(k, h)
                for a in range(nchunk):
                    if a > 0:
                        @pl.when(h == 0)
                        def _():
                            recv_row(k, a)
                    relax_block(k, a, h * half, half, ([first] if a < nchunk - 1 else []) + [own_cols(k + 1)], save=True)
                send_col(k + 1, h)
                return carry
            lax.fori_loop(0, HALVES, body, 0)
            rest(k, k + 1)

        @pl.when(jnp.logical_not(holder))
        def _():
            def body(h, carry):
                recv_col(k, h)
                for a in range(nchunk):
                    if a > 0:
                        @pl.when(h == 0)
                        def _():
                            recv_row(k, a)
                    relax_block(k, a, h * half, half, [slice(0 if a < nchunk - 1 else blk, dlo)])
                return carry
            lax.fori_loop(0, HALVES, body, 0)

    def round_body(k, carry):
        @pl.when(my_row == k)
        def _():
            @pl.when(k == 0)
            def _():
                recv_diag()
            own_turn(k)

            @pl.when((k + 1 < nrows) & (my_col == (k + 1) % ncols))
            def _():
                for h in range(HALVES):
                    send_col(k + 1, h)

        @pl.when(my_row == k + 1)
        def _():
            next_turn(k)

        @pl.when(my_row == k + 2)
        def _():
            second_turn(k)

        @pl.when(((my_row < k) & (k + 1 < nrows)) | (my_row > k + 2))
        def _():
            other_turn(k)

        @pl.when((my_row < k) & (k + 1 == nrows))
        def _():
            last_turn(k)
        return carry

    lax.fori_loop(0, nrows, round_body, 0)

    @pl.when(my_row + 1 == nrows)
    def _():
        for h in range(HALVES):
            store_half(h).start()

    @pl.when(my_col == my_row % ncols)
    def _():
        for h in range(HALVES):
            for d in range(1, ncols):
                diag_copy(h, d).wait_send()

    def drain(k, carry):
        @pl.when((my_col == k % ncols) & (my_row != k))
        def _():
            for h in range(HALVES):
                for d in range(1, ncols):
                    col_copy(k, h, d, d - 1).wait_send()
        for a in range(nchunk):
            @pl.when(fwd_here(k))
            def _():
                fwd_copy(k, a).wait_send()

            @pl.when(far_here(k, a))
            def _():
                far_copy(k, a).wait_send()
        return carry
    lax.fori_loop(0, nrows, drain, 0)
    for a in range(nchunk):
        for n in range(3):
            row_copy(my_row, a, n).wait_send()

        @pl.when(my_row + 1 == nrows)
        def _():
            row_copy(my_row, a, 3).wait_send()

        @pl.when((my_row + 1 < nrows) & (my_col == (my_row + 1) % ncols))
        def _():
            for d in range(1, ncols):
                nxt_copy(my_row, a, d).wait_send()
    for h in range(HALVES):
        store_half(h).wait()


def solution(mesh):
    nsub = mesh.shape['sub']
    nrows = mesh.shape['row'] * nsub
    ncols = mesh.shape['col']
    dist_spec = P(('parts', 'row', 'sub'), None, 'col')

    def local_run(local):
        rows_local, blk, own = local.shape
        assert rows_local == 1
        nchunk = blk // CHUNK
        nx = nrows // nsub
        dma = pltpu.SemaphoreType.DMA
        vmem = lambda *s: pltpu.VMEM(s, jnp.float32)
        return pl.pallas_call(
            functools.partial(kernel, nrows, ncols, nsub, blk),
            out_shape=jax.ShapeDtypeStruct(local.shape, local.dtype),
            in_specs=[pl.BlockSpec(memory_space=pl.ANY)],
            out_specs=pl.BlockSpec(memory_space=pl.ANY),
            scratch_shapes=[
                vmem(blk, own + 2 * blk), vmem(blk, blk), vmem(nrows, blk, blk),
                vmem(nrows, nchunk, CHUNK, own + 2 * blk), vmem(blk, blk, LANES), dma((HALVES,)),
                dma((nrows, HALVES, ncols - 1)), dma((nrows, HALVES)), dma((HALVES, ncols - 1)), dma((HALVES,)),
                dma((nchunk, 4)), dma((nrows, nchunk)), dma((nrows, nchunk, 2)),
                dma((nchunk, ncols - 1)), dma((nchunk,)),
            ],
            compiler_params=pltpu.CompilerParams(collective_id=0, has_side_effects=True, vmem_limit_bytes=16 * 2**20),
        )(local)

    return jax.shard_map(local_run, mesh=mesh, in_specs=(dist_spec,), out_specs=dist_spec, check_vma=False)
```

```python
import functools

import jax
import jax.numpy as jnp
from jax import lax
from jax.experimental import pallas as pl
from jax.experimental.pallas import tpu as pltpu
from jax.sharding import PartitionSpec as P

SUBL = 8
LANES = 128
CHUNK = 32
PAIRS = CHUNK // 2
STEP = 64
HALVES = 2
FULL = False


def relax(acc, src, cols, rows):
    for n, lane in enumerate(cols):
        acc = jnp.minimum(acc, jnp.broadcast_to(src[:, lane:lane + 1], acc.shape) + jnp.broadcast_to(rows(n), acc.shape))
    return acc


def lane_bcast(tile, lane):
    return jnp.broadcast_to(tile[:, lane:lane + 1], (tile.shape[0], LANES))


def widen(x, width):
    return jnp.concatenate([x] * (width // LANES), axis=1)


def lane_id(rows):
    return lax.broadcasted_iota(jnp.int32, (rows, LANES), 1)


def pair_bcast(tile, lanes):
    return jnp.take_along_axis(tile, lanes, axis=1, mode='promise_in_bounds')


def pair_lanes(rows):
    return jnp.where(lane_id(rows) < LANES // 2, 0, PAIRS)


def pack_rows(block):
    low = lane_id(PAIRS) < LANES // 2
    turned = pltpu.roll(block, LANES // 2, 1)
    return jnp.where(low, block[:PAIRS], turned[PAIRS:]), jnp.where(low, turned[:PAIRS], block[PAIRS:])


def kernel(nrows, ncols, nsub, blk, in_ref, out_ref, work, diag_in, colp, rowp, spread, io_sem,
           c_send, c_recv, s_send, s_recv, r_send, r_recv, f_send, n_send, n_recv):
    x = lax.axis_index('row')
    sub = lax.axis_index('sub')
    my_col = lax.axis_index('col')
    nx = nrows // nsub
    my_row = x * nsub + sub
    nchunk = blk // CHUNK
    half = blk // HALVES
    own = in_ref.shape[2]
    dlo = blk + own
    width = dlo + blk
    tiles = blk // SUBL
    tiles_per_chunk = CHUNK // SUBL

    def dev(row=None, col=None):
        out = {}
        if row is not None:
            out['row'] = row // nsub
            out['sub'] = row % nsub
        if col is not None:
            out['col'] = col
        return out

    def signal(target):
        pl.semaphore_signal(barrier, inc=1, device_id=target, device_id_type=pl.DeviceIdType.MESH)

    load_in = pltpu.make_async_copy(in_ref.at[0], work.at[:, blk:dlo], io_sem.at[0])
    load_in.start()
    barrier = pltpu.get_barrier_semaphore()
    for d in range(1, ncols):
        signal(dev(col=(my_col + d) % ncols))
    for d in range(1, nrows):
        signal(dev(row=(my_row + d) % nrows))
    for step, there in ((1, my_row + 1 < nrows), (-1, my_row > 0)):
        @pl.when(there)
        def _():
            for d in range(1, ncols):
                signal(dev(my_row + step, (my_col + d) % ncols))
    load_in.wait()
    middle = jnp.where((my_row > 0) & (my_row + 1 < nrows), 1, 0)
    pl.semaphore_wait(barrier, (2 + middle) * (ncols - 1) + nrows - 1)

    def remote(src, dst, ssem, rsem, target):
        return pltpu.make_async_remote_copy(src_ref=src, dst_ref=dst, send_sem=ssem, recv_sem=rsem,
                                            device_id=target, device_id_type=pl.DeviceIdType.MESH)

    def half_rows(h):
        return pl.ds(pl.multiple_of(h * half, half), half)

    def col_copy(k, h, d, n):
        part = colp.at[k, half_rows(h)]
        return remote(part, part, c_send.at[k, h, n], c_recv.at[k, h], dev(col=(my_col + d) % ncols))

    def diag_copy(h, d):
        part = diag_in.at[half_rows(h)]
        return remote(part, part, s_send.at[h, d - 1], s_recv.at[h], dev(col=(my_col + d) % ncols))

    def panel(k, a):
        lo = blk if a == nchunk - 1 else 0
        return rowp.at[k, a, :, lo:dlo]

    def row_copy(k, a, n):
        target = {'sub': (sub + 1) % nsub} if n == 0 else {'row': (x + (nx - 1, 1, 2)[n - 1]) % nx, 'sub': 0}
        return remote(panel(k, a), panel(k, a), r_send.at[a, n], r_recv.at[k, a], target)

    def fwd_copy(k, a):
        return remote(panel(k, a), panel(k, a), f_send.at[k, a, 0], r_recv.at[k, a], {'sub': (sub + 1) % nsub})

    def far_step(a):
        return 1 if a % 2 == 0 else nx - 1

    def far_copy(k, a):
        return remote(panel(k, a), panel(k, a), f_send.at[k, a, 1], r_recv.at[k, a], {'row': (x + far_step(a)) % nx, 'sub': 0})

    def fwd_here(k):
        return (sub == 0) & (x != k // nsub)

    def far_here(k, a):
        return (sub == 0) & (x == (k // nsub + far_step(a)) % nx) & (k + 1 < nrows)

    def nxt_copy(k, a, d):
        src = pl.ds(pl.multiple_of(blk + (k + 1) // ncols * blk, LANES), blk)
        return remote(rowp.at[k, a, :, src], rowp.at[k, a, :, dlo:width], n_send.at[a, d - 1], n_recv.at[a],
                      dev(k + 1, (my_col + d) % ncols))

    def own_cols(b):
        return pl.ds(pl.multiple_of(blk + b // ncols * blk, LANES), blk)

    def send_col(k, h):
        colp[k, half_rows(h)] = work[half_rows(h), own_cols(k)]
        for d in tuple(range(2, ncols - 1)) + (1, ncols - 1):
            col_copy(k, h, d, d - 1).start()

    def send_diag(h):
        diag_in[half_rows(h)] = work[half_rows(h), own_cols(my_row)]
        work[half_rows(h), dlo:width] = diag_in[half_rows(h)]
        for d in range(1, ncols):
            diag_copy(h, d).start()

    def recv_diag():
        @pl.when(my_col != my_row % ncols)
        def _():
            for h in range(HALVES):
                diag_copy(h, 1).wait_recv()
            work[:, dlo:width] = diag_in[...]

    def recv_col(k, h):
        @pl.when(my_col != k % ncols)
        def _():
            col_copy(k, h, 1, 0).wait_recv()
        work[half_rows(h), 0:blk] = colp[k, half_rows(h)]

    @pl.when((my_row <= 1) & (my_col == my_row % ncols))
    def _():
        for h in range(HALVES):
            send_diag(h)

    @pl.when((my_row != 0) & (my_col == 0))
    def _():
        for h in range(HALVES):
            send_col(0, h)

    def tile_rows(f, l):
        return slice(f * SUBL, l * SUBL)

    def close_chunk(k, a):
        dl = dlo - blk
        base = a * tiles_per_chunk
        vals = [work[tile_rows(base + t, base + t + 1), blk:width] for t in range(tiles_per_chunk)]
        for g in range(tiles_per_chunk):
            cols = [dl + (base + g) * SUBL + n for n in range(SUBL)]
            others = [t for t in range(tiles_per_chunk) if t != g]
            wide = jnp.concatenate([lane_bcast(vals[g], c) for c in cols] + [vals[g]], axis=1)
            spread = {t: [lane_bcast(vals[t], c) for c in cols] for t in others}
            for p in range(SUBL):
                piv, wide = wide[:, :LANES], wide[:, LANES:]
                wide = jnp.minimum(wide, widen(piv, wide.shape[1]) + jnp.broadcast_to(wide[p:p + 1, :], wide.shape))
            vals[g] = wide
            for t in others[g:] + others[:g]:
                for n in range(SUBL):
                    vals[t] = jnp.minimum(vals[t], widen(spread[t][n], own + blk) + jnp.broadcast_to(wide[n:n + 1, :], wide.shape))
        for t, v in enumerate(vals):
            work[tile_rows(base + t, base + t + 1), blk:width] = v
        for c in range(0, own + blk, LANES):
            packed = pack_rows(jnp.concatenate([v[:, c:c + LANES] for v in vals], axis=0))
            for n, v in enumerate(packed):
                r = slice(n * PAIRS, (n + 1) * PAIRS)
                rowp[k, a, r, blk + c:blk + c + LANES] = v
                if c == dl:
                    rowp[k, a, r, 0:blk] = v

    def send_chunk(k, a):
        sends_next = (k + 1 < nrows) & (my_col == (k + 1) % ncols)

        @pl.when(sends_next)
        def _():
            nxt_copy(k, a, 1).start()
        row_copy(k, a, 0).start()
        row_copy(k, a, 2).start()

        @pl.when(sends_next)
        def _():
            for d in range(2, ncols):
                nxt_copy(k, a, d).start()
        row_copy(k, a, 1).start()

        @pl.when(k + 1 == nrows)
        def _():
            row_copy(k, a, 3).start()

    def relax_by_chunk(a, f, l, step):
        for t in range(f, l, step):
            r = tile_rows(t, min(t + step, l))
            rows = lambda n: work[a * CHUNK + n:a * CHUNK + n + 1, blk:width]
            work[r, blk:width] = relax(work[r, blk:width], work[r, dlo:width], range(a * CHUNK, (a + 1) * CHUNK), rows)

    def spread_cols(a, f, l):
        r = tile_rows(f, l)
        src = work[r, dlo:width]
        for n in range(CHUNK):
            spread[n, r, :] = lane_bcast(src, a * CHUNK + n)

    def relax_spread(a, f, l):
        r = tile_rows(f, l)
        acc = work[r, blk:width]
        for n in range(CHUNK):
            row = work[a * CHUNK + n:a * CHUNK + n + 1, blk:width]
            acc = jnp.minimum(acc, widen(spread[n, r, :], own + blk) + jnp.broadcast_to(row, acc.shape))
        work[r, blk:width] = acc

    def own_turn(k):
        n = tiles_per_chunk

        close_chunk(k, 0)
        spread_cols(0, n, 2 * n)
        send_chunk(k, 0)
        relax_spread(0, n, 2 * n)
        close_chunk(k, 1)
        relax_by_chunk(0, 2 * n, 3 * n, n)
        spread_cols(1, 2 * n, 3 * n)
        send_chunk(k, 1)
        relax_spread(1, 2 * n, 3 * n)
        close_chunk(k, 2)
        relax_by_chunk(0, 3 * n, tiles, n)
        relax_by_chunk(1, 3 * n, tiles, n)
        spread_cols(2, 3 * n, tiles)
        send_chunk(k, 2)
        relax_spread(2, 3 * n, tiles)
        close_chunk(k, 3)
        send_chunk(k, 3)
        for a in range(1, nchunk):
            def body(it, carry):
                r = pl.ds(pl.multiple_of(it * CHUNK, CHUNK), CHUNK)
                rows = lambda n: work[a * CHUNK + n:a * CHUNK + n + 1, blk:width]
                work[r, blk:width] = relax(work[r, blk:width], work[r, dlo:width], range(a * CHUNK, (a + 1) * CHUNK), rows)
                return carry
            lax.fori_loop(0, a, body, 0)

    def recv_row(k, a):
        fwd_copy(k, a).wait_recv()

        @pl.when(fwd_here(k))
        def _():
            fwd_copy(k, a).start()

        @pl.when(far_here(k, a))
        def _():
            far_copy(k, a).start()

    def relax_block(k, chunks, start, count, sections, save=False, load=False):
        chunks = chunks if isinstance(chunks, tuple) else (chunks,)
        low = lane_id(STEP) < LANES // 2
        pairs = pair_lanes(STEP)
        sizes = [c.size if isinstance(c, pl.Slice) else c.stop - c.start for c in sections]
        for i in range(count // STEP):
            r = pl.ds(pl.multiple_of(start + i * STEP, STEP), STEP)
            src = None if load else work[r, 0:blk]
            accs = [None] * len(sections)
            for a, n in [(a, n) for a in chunks for n in range(PAIRS)]:
                if load:
                    wide = spread[a * PAIRS + n, r, :]
                else:
                    wide = pair_bcast(src, pairs + (a * CHUNK + n))
                if save:
                    spread[a * PAIRS + n, r, :] = wide
                for c, (cols, size) in enumerate(zip(sections, sizes)):
                    reps = widen(wide, size)
                    new = [reps + jnp.broadcast_to(rowp[k, a, m:m + 1, cols], reps.shape) for m in (n, n + PAIRS)]
                    accs[c] = new if accs[c] is None else [jnp.minimum(x, y) for x, y in zip(accs[c], new)]
            for (lower, upper), cols in zip(accs, sections):
                parts = []
                for b in range(0, lower.shape[1], LANES):
                    x, y = lower[:, b:b + LANES], upper[:, b:b + LANES]
                    parts.append(jnp.minimum(jnp.where(low, x, y), pltpu.roll(jnp.where(low, y, x), LANES // 2, 1)))
                work[r, cols] = jnp.minimum(work[r, cols], jnp.concatenate(parts, axis=1))


    first = slice(0, blk)

    def rest(k, b):
        other = pl.ds(pl.multiple_of(own - b // ncols * blk, LANES), blk)
        def body(h, carry):
            relax_block(k, tuple(range(nchunk)), h * half, half, [other], load=True)
            return carry
        lax.fori_loop(0, HALVES, body, 0)

    def next_turn(k):
        last = nchunk - 1

        def next_rows(a):
            holder = my_col == (k + 1) % ncols

            @pl.when(holder)
            def _():
                rowp[k, a, :, dlo:width] = rowp[k, a, :, own_cols(k + 1)]

            @pl.when(jnp.logical_not(holder))
            def _():
                nxt_copy(k, a, 1).wait_recv()

        recv_row(k, 0)

        def spread_last(h):
            src = work[half_rows(h), 0:blk]
            pairs = pair_lanes(half)
            for n in range(PAIRS):
                spread[last * PAIRS + n, half_rows(h), :] = pair_bcast(src, pairs + (last * CHUNK + n))

        @pl.when(sub >= 0)
        def _():
            def body(h, carry):
                recv_col(k, h)
                for a in range(last):
                    if a > 0:
                        @pl.when(h == 0)
                        def _():
                            recv_row(k, a)
                    relax_block(k, a, h * half, half, [slice(0, dlo)], save=True)
                spread_last(h)

                @pl.when((h == 0) & (sub == 0))
                def _():
                    recv_row(k, last)
                return carry
            lax.fori_loop(0, HALVES, body, 0)

        @pl.when(sub > 0)
        def _():
            recv_row(k, last)

        def finish(h, carry):
            relax_block(k, last, h * half, half, [slice(blk, dlo)], load=True)
            return carry
        lax.fori_loop(0, HALVES, finish, 0)
        recv_diag()
        for a in range(last):
            next_rows(a)
        relax_block(k, tuple(range(last)), 0, blk, [slice(dlo, width)], load=True)
        next_rows(last)
        relax_block(k, last, 0, blk, [slice(dlo, width)], load=True)

    def second_turn(k):
        sends_col = my_col == (k + 1) % ncols
        sends_diag = my_col == (k + 2) % ncols
        block = jnp.where(sends_col, k + 1, k + 2)
        recv_row(k, 0)

        def half_turn(h, sections, save):
            recv_col(k, h)
            for a in range(nchunk):
                if a > 0:
                    @pl.when(h == 0)
                    def _():
                        recv_row(k, a)
                relax_block(k, a, h * half, half, sections(a), save=save)

        @pl.when(sends_col | sends_diag)
        def _():
            def body(h, carry):
                half_turn(h, lambda a: ([first] if a < nchunk - 1 else []) + [own_cols(block)], True)

                @pl.when(sends_col)
                def _():
                    send_col(k + 1, h)

                @pl.when(sends_diag)
                def _():
                    send_diag(h)
                return carry
            lax.fori_loop(0, HALVES, body, 0)
            rest(k, block)

        @pl.when(jnp.logical_not(sends_col | sends_diag))
        def _():
            def body(h, carry):
                half_turn(h, lambda a: [slice(0 if a < nchunk - 1 else blk, dlo)], False)
                return carry
            lax.fori_loop(0, HALVES, body, 0)

    def store_half(h):
        return pltpu.make_async_copy(work.at[half_rows(h), blk:dlo], out_ref.at[0, half_rows(h)], io_sem.at[h])

    def last_turn(k):
        recv_row(k, 0)

        def body(h, carry):
            recv_col(k, h)
            for a in range(nchunk):
                if a > 0:
                    @pl.when(h == 0)
                    def _():
                        recv_row(k, a)
                relax_block(k, a, h * half, half, [slice(0 if a < nchunk - 1 else blk, dlo)])
            store_half(h).start()
            return carry
        lax.fori_loop(0, HALVES, body, 0)

    def other_turn(k):
        holder = (k + 1 < nrows) & (my_col == (k + 1) % ncols)
        recv_row(k, 0)

        @pl.when(holder)
        def _():
            def body(h, carry):
                recv_col(k, h)
                for a in range(nchunk):
                    if a > 0:
                        @pl.when(h == 0)
                        def _():
                            recv_row(k, a)
                    relax_block(k, a, h * half, half, ([first] if a < nchunk - 1 else []) + [own_cols(k + 1)], save=True)
                send_col(k + 1, h)
                return carry
            lax.fori_loop(0, HALVES, body, 0)
            rest(k, k + 1)

        @pl.when(jnp.logical_not(holder))
        def _():
            def body(h, carry):
                recv_col(k, h)
                for a in range(nchunk):
                    if a > 0:
                        @pl.when(h == 0)
                        def _():
                            recv_row(k, a)
                    relax_block(k, a, h * half, half, [slice(0 if a < nchunk - 1 else blk, dlo)])
                return carry
            lax.fori_loop(0, HALVES, body, 0)

    def round_body(k, carry):
        @pl.when(my_row == k)
        def _():
            @pl.when(k == 0)
            def _():
                recv_diag()
            own_turn(k)

            @pl.when((k + 1 < nrows) & (my_col == (k + 1) % ncols))
            def _():
                for h in range(HALVES):
                    send_col(k + 1, h)

        @pl.when(my_row == k + 1)
        def _():
            next_turn(k)

        @pl.when(my_row == k + 2)
        def _():
            second_turn(k)

        @pl.when(((my_row < k) & (k + 1 < nrows)) | (my_row > k + 2))
        def _():
            other_turn(k)

        @pl.when((my_row < k) & (k + 1 == nrows))
        def _():
            last_turn(k)
        return carry

    lax.fori_loop(0, nrows, round_body, 0)

    @pl.when(my_row + 1 == nrows)
    def _():
        for h in range(HALVES):
            store_half(h).start()

    @pl.when(my_col == my_row % ncols)
    def _():
        for h in range(HALVES):
            for d in range(1, ncols):
                diag_copy(h, d).wait_send()

    def drain(k, carry):
        @pl.when((my_col == k % ncols) & (my_row != k))
        def _():
            for h in range(HALVES):
                for d in range(1, ncols):
                    col_copy(k, h, d, d - 1).wait_send()
        for a in range(nchunk):
            @pl.when(fwd_here(k))
            def _():
                fwd_copy(k, a).wait_send()

            @pl.when(far_here(k, a))
            def _():
                far_copy(k, a).wait_send()
        return carry
    lax.fori_loop(0, nrows, drain, 0)
    for a in range(nchunk):
        for n in range(3):
            row_copy(my_row, a, n).wait_send()

        @pl.when(my_row + 1 == nrows)
        def _():
            row_copy(my_row, a, 3).wait_send()

        @pl.when((my_row + 1 < nrows) & (my_col == (my_row + 1) % ncols))
        def _():
            for d in range(1, ncols):
                nxt_copy(my_row, a, d).wait_send()
    for h in range(HALVES):
        store_half(h).wait()


def solution(mesh):
    nsub = mesh.shape['sub']
    nrows = mesh.shape['row'] * nsub
    ncols = mesh.shape['col']
    dist_spec = P(('parts', 'row', 'sub'), None, 'col')

    def local_run(local):
        rows_local, blk, own = local.shape
        assert rows_local == 1
        nchunk = blk // CHUNK
        nx = nrows // nsub
        dma = pltpu.SemaphoreType.DMA
        vmem = lambda *s: pltpu.VMEM(s, jnp.float32)
        return pl.pallas_call(
            functools.partial(kernel, nrows, ncols, nsub, blk),
            out_shape=jax.ShapeDtypeStruct(local.shape, local.dtype),
            in_specs=[pl.BlockSpec(memory_space=pl.ANY)],
            out_specs=pl.BlockSpec(memory_space=pl.ANY),
            scratch_shapes=[
                vmem(blk, own + 2 * blk), vmem(blk, blk), vmem(nrows, blk, blk),
                vmem(nrows, nchunk, CHUNK, own + 2 * blk), vmem(blk, blk, LANES), dma((HALVES,)),
                dma((nrows, HALVES, ncols - 1)), dma((nrows, HALVES)), dma((HALVES, ncols - 1)), dma((HALVES,)),
                dma((nchunk, 4)), dma((nrows, nchunk)), dma((nrows, nchunk, 2)),
                dma((nchunk, ncols - 1)), dma((nchunk,)),
            ],
            compiler_params=pltpu.CompilerParams(collective_id=0, has_side_effects=True, vmem_limit_bytes=16 * 2**20),
        )(local)

    return jax.shard_map(local_run, mesh=mesh, in_specs=(dist_spec,), out_specs=dist_spec, check_vma=False)
```

```python
import functools

import jax
import jax.numpy as jnp
from jax import lax
from jax.experimental import pallas as pl
from jax.experimental.pallas import tpu as pltpu
from jax.sharding import PartitionSpec as P

SUBL = 8
LANES = 128
CHUNK = 32
PAIRS = CHUNK // 2
STEP = 64
HALVES = 2
FULL = False


def relax(acc, src, cols, rows):
    for n, lane in enumerate(cols):
        acc = jnp.minimum(acc, jnp.broadcast_to(src[:, lane:lane + 1], acc.shape) + jnp.broadcast_to(rows(n), acc.shape))
    return acc


def lane_bcast(tile, lane):
    return jnp.broadcast_to(tile[:, lane:lane + 1], (tile.shape[0], LANES))


def widen(x, width):
    return jnp.concatenate([x] * (width // LANES), axis=1)


def lane_id(rows):
    return lax.broadcasted_iota(jnp.int32, (rows, LANES), 1)


def pair_bcast(tile, lanes):
    return jnp.take_along_axis(tile, lanes, axis=1, mode='promise_in_bounds')


def pair_lanes(rows):
    return jnp.where(lane_id(rows) < LANES // 2, 0, PAIRS)


def pack_rows(block):
    low = lane_id(PAIRS) < LANES // 2
    turned = pltpu.roll(block, LANES // 2, 1)
    return jnp.where(low, block[:PAIRS], turned[PAIRS:]), jnp.where(low, turned[:PAIRS], block[PAIRS:])


def kernel(nrows, ncols, nsub, blk, in_ref, out_ref, work, diag_in, colp, rowp, spread, io_sem,
           c_send, c_recv, s_send, s_recv, r_send, r_recv, f_send, n_send, n_recv):
    x = lax.axis_index('row')
    sub = lax.axis_index('sub')
    my_col = lax.axis_index('col')
    nx = nrows // nsub
    my_row = x * nsub + sub
    nchunk = blk // CHUNK
    half = blk // HALVES
    own = in_ref.shape[2]
    dlo = blk + own
    width = dlo + blk
    tiles = blk // SUBL
    tiles_per_chunk = CHUNK // SUBL

    def dev(row=None, col=None):
        out = {}
        if row is not None:
            out['row'] = row // nsub
            out['sub'] = row % nsub
        if col is not None:
            out['col'] = col
        return out

    def signal(target):
        pl.semaphore_signal(barrier, inc=1, device_id=target, device_id_type=pl.DeviceIdType.MESH)

    load_in = pltpu.make_async_copy(in_ref.at[0], work.at[:, blk:dlo], io_sem.at[0])
    load_in.start()
    barrier = pltpu.get_barrier_semaphore()
    for d in range(1, ncols):
        signal(dev(col=(my_col + d) % ncols))
    for d in range(1, nrows):
        signal(dev(row=(my_row + d) % nrows))
    for step, there in ((1, my_row + 1 < nrows), (-1, my_row > 0)):
        @pl.when(there)
        def _():
            for d in range(1, ncols):
                signal(dev(my_row + step, (my_col + d) % ncols))
    load_in.wait()
    middle = jnp.where((my_row > 0) & (my_row + 1 < nrows), 1, 0)
    pl.semaphore_wait(barrier, (2 + middle) * (ncols - 1) + nrows - 1)

    def remote(src, dst, ssem, rsem, target):
        return pltpu.make_async_remote_copy(src_ref=src, dst_ref=dst, send_sem=ssem, recv_sem=rsem,
                                            device_id=target, device_id_type=pl.DeviceIdType.MESH)

    def half_rows(h):
        return pl.ds(pl.multiple_of(h * half, half), half)

    def col_copy(k, h, d, n):
        part = colp.at[k, half_rows(h)]
        return remote(part, part, c_send.at[k, h, n], c_recv.at[k, h], dev(col=(my_col + d) % ncols))

    def diag_copy(h, d):
        part = diag_in.at[half_rows(h)]
        return remote(part, part, s_send.at[h, d - 1], s_recv.at[h], dev(col=(my_col + d) % ncols))

    def panel(k, a):
        lo = blk if a == nchunk - 1 else 0
        return rowp.at[k, a, :, lo:dlo]

    def row_copy(k, a, n):
        target = {'sub': (sub + 1) % nsub} if n == 0 else {'row': (x + (nx - 1, 1, 2)[n - 1]) % nx, 'sub': 0}
        return remote(panel(k, a), panel(k, a), r_send.at[a, n], r_recv.at[k, a], target)

    def fwd_copy(k, a):
        return remote(panel(k, a), panel(k, a), f_send.at[k, a, 0], r_recv.at[k, a], {'sub': (sub + 1) % nsub})

    def far_step(a):
        return 1 if a % 2 == 0 else nx - 1

    def far_copy(k, a):
        return remote(panel(k, a), panel(k, a), f_send.at[k, a, 1], r_recv.at[k, a], {'row': (x + far_step(a)) % nx, 'sub': 0})

    def fwd_here(k):
        return (sub == 0) & (x != k // nsub)

    def far_here(k, a):
        return (sub == 0) & (x == (k // nsub + far_step(a)) % nx) & (k + 1 < nrows)

    def nxt_copy(k, a, d):
        src = pl.ds(pl.multiple_of(blk + (k + 1) // ncols * blk, LANES), blk)
        return remote(rowp.at[k, a, :, src], rowp.at[k, a, :, dlo:width], n_send.at[a, d - 1], n_recv.at[a],
                      dev(k + 1, (my_col + d) % ncols))

    def own_cols(b):
        return pl.ds(pl.multiple_of(blk + b // ncols * blk, LANES), blk)

    def send_col(k, h):
        colp[k, half_rows(h)] = work[half_rows(h), own_cols(k)]
        for d in tuple(range(2, ncols - 1)) + (1, ncols - 1):
            col_copy(k, h, d, d - 1).start()

    def send_diag(h):
        diag_in[half_rows(h)] = work[half_rows(h), own_cols(my_row)]
        work[half_rows(h), dlo:width] = diag_in[half_rows(h)]
        for d in range(1, ncols):
            diag_copy(h, d).start()

    def recv_diag():
        @pl.when(my_col != my_row % ncols)
        def _():
            for h in range(HALVES):
                diag_copy(h, 1).wait_recv()
            work[:, dlo:width] = diag_in[...]

    def recv_col(k, h):
        @pl.when(my_col != k % ncols)
        def _():
            col_copy(k, h, 1, 0).wait_recv()
        work[half_rows(h), 0:blk] = colp[k, half_rows(h)]

    @pl.when((my_row <= 1) & (my_col == my_row % ncols))
    def _():
        for h in range(HALVES):
            send_diag(h)

    @pl.when((my_row != 0) & (my_col == 0))
    def _():
        for h in range(HALVES):
            send_col(0, h)

    def tile_rows(f, l):
        return slice(f * SUBL, l * SUBL)

    def close_chunk(k, a):
        dl = dlo - blk
        base = a * tiles_per_chunk
        vals = [work[tile_rows(base + t, base + t + 1), blk:width] for t in range(tiles_per_chunk)]
        for g in range(tiles_per_chunk):
            cols = [dl + (base + g) * SUBL + n for n in range(SUBL)]
            others = [t for t in range(tiles_per_chunk) if t != g]
            wide = jnp.concatenate([lane_bcast(vals[g], c) for c in cols] + [vals[g]], axis=1)
            spread = {t: [lane_bcast(vals[t], c) for c in cols] for t in others}
            for p in range(SUBL):
                piv, wide = wide[:, :LANES], wide[:, LANES:]
                wide = jnp.minimum(wide, widen(piv, wide.shape[1]) + jnp.broadcast_to(wide[p:p + 1, :], wide.shape))
            vals[g] = wide
            for t in others[g:] + others[:g]:
                for n in range(SUBL):
                    vals[t] = jnp.minimum(vals[t], widen(spread[t][n], own + blk) + jnp.broadcast_to(wide[n:n + 1, :], wide.shape))
        for t, v in enumerate(vals):
            work[tile_rows(base + t, base + t + 1), blk:width] = v
        for c in range(0, own + blk, LANES):
            packed = pack_rows(jnp.concatenate([v[:, c:c + LANES] for v in vals], axis=0))
            for n, v in enumerate(packed):
                r = slice(n * PAIRS, (n + 1) * PAIRS)
                rowp[k, a, r, blk + c:blk + c + LANES] = v
                if c == dl:
                    rowp[k, a, r, 0:blk] = v

    def send_chunk(k, a):
        sends_next = (k + 1 < nrows) & (my_col == (k + 1) % ncols)

        row_copy(k, a, 0).start()
        row_copy(k, a, 2).start()
        row_copy(k, a, 1).start()

        @pl.when(sends_next)
        def _():
            for d in tuple(range(2, ncols - 1)) + (1, ncols - 1):
                nxt_copy(k, a, d).start()

        @pl.when(k + 1 == nrows)
        def _():
            row_copy(k, a, 3).start()

    def relax_by_chunk(a, f, l, step):
        for t in range(f, l, step):
            r = tile_rows(t, min(t + step, l))
            rows = lambda n: work[a * CHUNK + n:a * CHUNK + n + 1, blk:width]
            work[r, blk:width] = relax(work[r, blk:width], work[r, dlo:width], range(a * CHUNK, (a + 1) * CHUNK), rows)

    def spread_cols(a, f, l):
        r = tile_rows(f, l)
        src = work[r, dlo:width]
        for n in range(CHUNK):
            spread[n, r, :] = lane_bcast(src, a * CHUNK + n)

    def relax_spread(a, f, l):
        r = tile_rows(f, l)
        acc = work[r, blk:width]
        for n in range(CHUNK):
            row = work[a * CHUNK + n:a * CHUNK + n + 1, blk:width]
            acc = jnp.minimum(acc, widen(spread[n, r, :], own + blk) + jnp.broadcast_to(row, acc.shape))
        work[r, blk:width] = acc

    def own_turn(k):
        n = tiles_per_chunk

        close_chunk(k, 0)
        spread_cols(0, n, 2 * n)
        send_chunk(k, 0)
        relax_spread(0, n, 2 * n)
        close_chunk(k, 1)
        relax_by_chunk(0, 2 * n, 3 * n, n)
        spread_cols(1, 2 * n, 3 * n)
        send_chunk(k, 1)
        relax_spread(1, 2 * n, 3 * n)
        close_chunk(k, 2)
        relax_by_chunk(0, 3 * n, tiles, n)
        relax_by_chunk(1, 3 * n, tiles, n)
        spread_cols(2, 3 * n, tiles)
        send_chunk(k, 2)
        relax_spread(2, 3 * n, tiles)
        close_chunk(k, 3)
        send_chunk(k, 3)
        for a in range(1, nchunk):
            def body(it, carry):
                r = pl.ds(pl.multiple_of(it * CHUNK, CHUNK), CHUNK)
                rows = lambda n: work[a * CHUNK + n:a * CHUNK + n + 1, blk:width]
                work[r, blk:width] = relax(work[r, blk:width], work[r, dlo:width], range(a * CHUNK, (a + 1) * CHUNK), rows)
                return carry
            lax.fori_loop(0, a, body, 0)

    def recv_row(k, a):
        fwd_copy(k, a).wait_recv()

        @pl.when(fwd_here(k))
        def _():
            fwd_copy(k, a).start()

        @pl.when(far_here(k, a))
        def _():
            far_copy(k, a).start()

    def relax_block(k, chunks, start, count, sections, save=False, load=False):
        chunks = chunks if isinstance(chunks, tuple) else (chunks,)
        low = lane_id(STEP) < LANES // 2
        pairs = pair_lanes(STEP)
        sizes = [c.size if isinstance(c, pl.Slice) else c.stop - c.start for c in sections]
        for i in range(count // STEP):
            r = pl.ds(pl.multiple_of(start + i * STEP, STEP), STEP)
            src = None if load else work[r, 0:blk]
            accs = [None] * len(sections)
            for a, n in [(a, n) for a in chunks for n in range(PAIRS)]:
                if load:
                    wide = spread[a * PAIRS + n, r, :]
                else:
                    wide = pair_bcast(src, pairs + (a * CHUNK + n))
                if save:
                    spread[a * PAIRS + n, r, :] = wide
                for c, (cols, size) in enumerate(zip(sections, sizes)):
                    reps = widen(wide, size)
                    new = [reps + jnp.broadcast_to(rowp[k, a, m:m + 1, cols], reps.shape) for m in (n, n + PAIRS)]
                    accs[c] = new if accs[c] is None else [jnp.minimum(x, y) for x, y in zip(accs[c], new)]
            for (lower, upper), cols in zip(accs, sections):
                parts = []
                for b in range(0, lower.shape[1], LANES):
                    x, y = lower[:, b:b + LANES], upper[:, b:b + LANES]
                    parts.append(jnp.minimum(jnp.where(low, x, y), pltpu.roll(jnp.where(low, y, x), LANES // 2, 1)))
                work[r, cols] = jnp.minimum(work[r, cols], jnp.concatenate(parts, axis=1))


    first = slice(0, blk)

    def rest(k, b):
        other = pl.ds(pl.multiple_of(own - b // ncols * blk, LANES), blk)
        def body(h, carry):
            relax_block(k, tuple(range(nchunk)), h * half, half, [other], load=True)
            return carry
        lax.fori_loop(0, HALVES, body, 0)

    def next_turn(k):
        last = nchunk - 1

        def next_rows(a):
            holder = my_col == (k + 1) % ncols

            @pl.when(holder)
            def _():
                rowp[k, a, :, dlo:width] = rowp[k, a, :, own_cols(k + 1)]

            @pl.when(jnp.logical_not(holder))
            def _():
                nxt_copy(k, a, 1).wait_recv()

        recv_row(k, 0)

        def spread_last(h):
            src = work[half_rows(h), 0:blk]
            pairs = pair_lanes(half)
            for n in range(PAIRS):
                spread[last * PAIRS + n, half_rows(h), :] = pair_bcast(src, pairs + (last * CHUNK + n))

        @pl.when(sub >= 0)
        def _():
            def body(h, carry):
                recv_col(k, h)
                for a in range(last):
                    if a > 0:
                        @pl.when(h == 0)
                        def _():
                            recv_row(k, a)
                    relax_block(k, a, h * half, half, [slice(0, dlo)], save=True)
                spread_last(h)

                @pl.when((h == 0) & (sub == 0))
                def _():
                    recv_row(k, last)
                return carry
            lax.fori_loop(0, HALVES, body, 0)

        @pl.when(sub > 0)
        def _():
            recv_row(k, last)

        def finish(h, carry):
            relax_block(k, last, h * half, half, [slice(blk, dlo)], load=True)
            return carry
        lax.fori_loop(0, HALVES, finish, 0)
        recv_diag()
        for a in range(last):
            next_rows(a)
        relax_block(k, tuple(range(last)), 0, blk, [slice(dlo, width)], load=True)
        next_rows(last)
        relax_block(k, last, 0, blk, [slice(dlo, width)], load=True)

    def second_turn(k):
        sends_col = my_col == (k + 1) % ncols
        sends_diag = my_col == (k + 2) % ncols
        block = jnp.where(sends_col, k + 1, k + 2)
        recv_row(k, 0)

        def half_turn(h, sections, save):
            recv_col(k, h)
            for a in range(nchunk):
                if a > 0:
                    @pl.when(h == 0)
                    def _():
                        recv_row(k, a)
                relax_block(k, a, h * half, half, sections(a), save=save)

        @pl.when(sends_col | sends_diag)
        def _():
            def body(h, carry):
                half_turn(h, lambda a: ([first] if a < nchunk - 1 else []) + [own_cols(block)], True)

                @pl.when(sends_col)
                def _():
                    send_col(k + 1, h)

                @pl.when(sends_diag)
                def _():
                    send_diag(h)
                return carry
            lax.fori_loop(0, HALVES, body, 0)
            rest(k, block)

        @pl.when(jnp.logical_not(sends_col | sends_diag))
        def _():
            def body(h, carry):
                half_turn(h, lambda a: [slice(0 if a < nchunk - 1 else blk, dlo)], False)
                return carry
            lax.fori_loop(0, HALVES, body, 0)

    def store_half(h):
        return pltpu.make_async_copy(work.at[half_rows(h), blk:dlo], out_ref.at[0, half_rows(h)], io_sem.at[h])

    def last_turn(k):
        recv_row(k, 0)

        def body(h, carry):
            recv_col(k, h)
            for a in range(nchunk):
                if a > 0:
                    @pl.when(h == 0)
                    def _():
                        recv_row(k, a)
                relax_block(k, a, h * half, half, [slice(0 if a < nchunk - 1 else blk, dlo)])
            store_half(h).start()
            return carry
        lax.fori_loop(0, HALVES, body, 0)

    def other_turn(k):
        holder = (k + 1 < nrows) & (my_col == (k + 1) % ncols)
        recv_row(k, 0)

        @pl.when(holder)
        def _():
            def body(h, carry):
                recv_col(k, h)
                for a in range(nchunk):
                    if a > 0:
                        @pl.when(h == 0)
                        def _():
                            recv_row(k, a)
                    relax_block(k, a, h * half, half, ([first] if a < nchunk - 1 else []) + [own_cols(k + 1)], save=True)
                send_col(k + 1, h)
                return carry
            lax.fori_loop(0, HALVES, body, 0)
            rest(k, k + 1)

        @pl.when(jnp.logical_not(holder))
        def _():
            def body(h, carry):
                recv_col(k, h)
                for a in range(nchunk):
                    if a > 0:
                        @pl.when(h == 0)
                        def _():
                            recv_row(k, a)
                    relax_block(k, a, h * half, half, [slice(0 if a < nchunk - 1 else blk, dlo)])
                return carry
            lax.fori_loop(0, HALVES, body, 0)

    def round_body(k, carry):
        @pl.when(my_row == k)
        def _():
            @pl.when(k == 0)
            def _():
                recv_diag()
            own_turn(k)

            @pl.when((k + 1 < nrows) & (my_col == (k + 1) % ncols))
            def _():
                for h in range(HALVES):
                    send_col(k + 1, h)

        @pl.when(my_row == k + 1)
        def _():
            next_turn(k)

        @pl.when(my_row == k + 2)
        def _():
            second_turn(k)

        @pl.when(((my_row < k) & (k + 1 < nrows)) | (my_row > k + 2))
        def _():
            other_turn(k)

        @pl.when((my_row < k) & (k + 1 == nrows))
        def _():
            last_turn(k)
        return carry

    lax.fori_loop(0, nrows, round_body, 0)

    @pl.when(my_row + 1 == nrows)
    def _():
        for h in range(HALVES):
            store_half(h).start()

    @pl.when(my_col == my_row % ncols)
    def _():
        for h in range(HALVES):
            for d in range(1, ncols):
                diag_copy(h, d).wait_send()

    def drain(k, carry):
        @pl.when((my_col == k % ncols) & (my_row != k))
        def _():
            for h in range(HALVES):
                for d in range(1, ncols):
                    col_copy(k, h, d, d - 1).wait_send()
        for a in range(nchunk):
            @pl.when(fwd_here(k))
            def _():
                fwd_copy(k, a).wait_send()

            @pl.when(far_here(k, a))
            def _():
                far_copy(k, a).wait_send()
        return carry
    lax.fori_loop(0, nrows, drain, 0)
    for a in range(nchunk):
        for n in range(3):
            row_copy(my_row, a, n).wait_send()

        @pl.when(my_row + 1 == nrows)
        def _():
            row_copy(my_row, a, 3).wait_send()

        @pl.when((my_row + 1 < nrows) & (my_col == (my_row + 1) % ncols))
        def _():
            for d in range(1, ncols):
                nxt_copy(my_row, a, d).wait_send()
    for h in range(HALVES):
        store_half(h).wait()


def solution(mesh):
    nsub = mesh.shape['sub']
    nrows = mesh.shape['row'] * nsub
    ncols = mesh.shape['col']
    dist_spec = P(('parts', 'row', 'sub'), None, 'col')

    def local_run(local):
        rows_local, blk, own = local.shape
        assert rows_local == 1
        nchunk = blk // CHUNK
        nx = nrows // nsub
        dma = pltpu.SemaphoreType.DMA
        vmem = lambda *s: pltpu.VMEM(s, jnp.float32)
        return pl.pallas_call(
            functools.partial(kernel, nrows, ncols, nsub, blk),
            out_shape=jax.ShapeDtypeStruct(local.shape, local.dtype),
            in_specs=[pl.BlockSpec(memory_space=pl.ANY)],
            out_specs=pl.BlockSpec(memory_space=pl.ANY),
            scratch_shapes=[
                vmem(blk, own + 2 * blk), vmem(blk, blk), vmem(nrows, blk, blk),
                vmem(nrows, nchunk, CHUNK, own + 2 * blk), vmem(blk, blk, LANES), dma((HALVES,)),
                dma((nrows, HALVES, ncols - 1)), dma((nrows, HALVES)), dma((HALVES, ncols - 1)), dma((HALVES,)),
                dma((nchunk, 4)), dma((nrows, nchunk)), dma((nrows, nchunk, 2)),
                dma((nchunk, ncols - 1)), dma((nchunk,)),
            ],
            compiler_params=pltpu.CompilerParams(collective_id=0, has_side_effects=True, vmem_limit_bytes=16 * 2**20),
        )(local)

    return jax.shard_map(local_run, mesh=mesh, in_specs=(dist_spec,), out_specs=dist_spec, check_vma=False)
```

```python
import functools

import jax
import jax.numpy as jnp
from jax import lax
from jax.experimental import pallas as pl
from jax.experimental.pallas import tpu as pltpu
from jax.sharding import PartitionSpec as P

SUBL = 8
LANES = 128
CHUNK = 32
PAIRS = CHUNK // 2
STEP = 64
HALVES = 2
FULL = False


def relax(acc, src, cols, rows):
    for n, lane in enumerate(cols):
        acc = jnp.minimum(acc, jnp.broadcast_to(src[:, lane:lane + 1], acc.shape) + jnp.broadcast_to(rows(n), acc.shape))
    return acc


def lane_bcast(tile, lane):
    return jnp.broadcast_to(tile[:, lane:lane + 1], (tile.shape[0], LANES))


def widen(x, width):
    return jnp.concatenate([x] * (width // LANES), axis=1)


def lane_id(rows):
    return lax.broadcasted_iota(jnp.int32, (rows, LANES), 1)


def pair_bcast(tile, lanes):
    return jnp.take_along_axis(tile, lanes, axis=1, mode='promise_in_bounds')


def pair_lanes(rows):
    return jnp.where(lane_id(rows) < LANES // 2, 0, PAIRS)


def pack_rows(block):
    low = lane_id(PAIRS) < LANES // 2
    turned = pltpu.roll(block, LANES // 2, 1)
    return jnp.where(low, block[:PAIRS], turned[PAIRS:]), jnp.where(low, turned[:PAIRS], block[PAIRS:])


def kernel(nrows, ncols, nsub, blk, in_ref, out_ref, work, diag_in, colp, rowp, spread, io_sem,
           c_send, c_recv, s_send, s_recv, r_send, r_recv, f_send, n_send, n_recv):
    x = lax.axis_index('row')
    sub = lax.axis_index('sub')
    my_col = lax.axis_index('col')
    nx = nrows // nsub
    my_row = x * nsub + sub
    nchunk = blk // CHUNK
    half = blk // HALVES
    own = in_ref.shape[2]
    dlo = blk + own
    width = dlo + blk
    tiles = blk // SUBL
    tiles_per_chunk = CHUNK // SUBL

    def dev(row=None, col=None):
        out = {}
        if row is not None:
            out['row'] = row // nsub
            out['sub'] = row % nsub
        if col is not None:
            out['col'] = col
        return out

    def signal(target):
        pl.semaphore_signal(barrier, inc=1, device_id=target, device_id_type=pl.DeviceIdType.MESH)

    load_in = pltpu.make_async_copy(in_ref.at[0], work.at[:, blk:dlo], io_sem.at[0])
    load_in.start()
    barrier = pltpu.get_barrier_semaphore()
    for d in range(1, ncols):
        signal(dev(col=(my_col + d) % ncols))
    for d in range(1, nrows):
        signal(dev(row=(my_row + d) % nrows))
    for step, there in ((1, my_row + 1 < nrows), (-1, my_row > 0)):
        @pl.when(there)
        def _():
            for d in range(1, ncols):
                signal(dev(my_row + step, (my_col + d) % ncols))
    load_in.wait()
    middle = jnp.where((my_row > 0) & (my_row + 1 < nrows), 1, 0)
    pl.semaphore_wait(barrier, (2 + middle) * (ncols - 1) + nrows - 1)

    def remote(src, dst, ssem, rsem, target):
        return pltpu.make_async_remote_copy(src_ref=src, dst_ref=dst, send_sem=ssem, recv_sem=rsem,
                                            device_id=target, device_id_type=pl.DeviceIdType.MESH)

    def half_rows(h):
        return pl.ds(pl.multiple_of(h * half, half), half)

    def col_copy(k, h, d, n):
        part = colp.at[k, half_rows(h)]
        return remote(part, part, c_send.at[k, h, n], c_recv.at[k, h], dev(col=(my_col + d) % ncols))

    def diag_copy(h, d):
        part = diag_in.at[half_rows(h)]
        return remote(part, part, s_send.at[h, d - 1], s_recv.at[h], dev(col=(my_col + d) % ncols))

    def panel(k, a):
        lo = blk if a == nchunk - 1 else 0
        return rowp.at[k, a, :, lo:dlo]

    def row_copy(k, a, n):
        target = {'sub': (sub + 1) % nsub} if n == 0 else {'row': (x + (nx - 1, 1, 2)[n - 1]) % nx, 'sub': 0}
        return remote(panel(k, a), panel(k, a), r_send.at[a, n], r_recv.at[k, a], target)

    def fwd_copy(k, a):
        return remote(panel(k, a), panel(k, a), f_send.at[k, a, 0], r_recv.at[k, a], {'sub': (sub + 1) % nsub})

    def far_step(a):
        return 1 if a % 2 == 0 else nx - 1

    def far_copy(k, a):
        return remote(panel(k, a), panel(k, a), f_send.at[k, a, 1], r_recv.at[k, a], {'row': (x + far_step(a)) % nx, 'sub': 0})

    def fwd_here(k):
        return (sub == 0) & (x != k // nsub)

    def far_here(k, a):
        return (sub == 0) & (x == (k // nsub + far_step(a)) % nx) & (k + 1 < nrows)

    def nxt_copy(k, a, d):
        src = pl.ds(pl.multiple_of(blk + (k + 1) // ncols * blk, LANES), blk)
        return remote(rowp.at[k, a, :, src], rowp.at[k, a, :, dlo:width], n_send.at[a, d - 1], n_recv.at[a],
                      dev(k + 1, (my_col + d) % ncols))

    def own_cols(b):
        return pl.ds(pl.multiple_of(blk + b // ncols * blk, LANES), blk)

    def send_col(k, h):
        colp[k, half_rows(h)] = work[half_rows(h), own_cols(k)]
        for d in tuple(range(2, ncols - 1)) + (1, ncols - 1):
            col_copy(k, h, d, d - 1).start()

    def send_diag(h):
        diag_in[half_rows(h)] = work[half_rows(h), own_cols(my_row)]
        work[half_rows(h), dlo:width] = diag_in[half_rows(h)]
        for d in range(1, ncols):
            diag_copy(h, d).start()

    def recv_diag():
        @pl.when(my_col != my_row % ncols)
        def _():
            for h in range(HALVES):
                diag_copy(h, 1).wait_recv()
            work[:, dlo:width] = diag_in[...]

    def recv_col(k, h):
        @pl.when(my_col != k % ncols)
        def _():
            col_copy(k, h, 1, 0).wait_recv()
        work[half_rows(h), 0:blk] = colp[k, half_rows(h)]

    @pl.when((my_row <= 1) & (my_col == my_row % ncols))
    def _():
        for h in range(HALVES):
            send_diag(h)

    @pl.when((my_row != 0) & (my_col == 0))
    def _():
        for h in range(HALVES):
            send_col(0, h)

    def tile_rows(f, l):
        return slice(f * SUBL, l * SUBL)

    def close_chunk(k, a):
        dl = dlo - blk
        base = a * tiles_per_chunk
        vals = [work[tile_rows(base + t, base + t + 1), blk:width] for t in range(tiles_per_chunk)]
        for g in range(tiles_per_chunk):
            cols = [dl + (base + g) * SUBL + n for n in range(SUBL)]
            others = [t for t in range(tiles_per_chunk) if t != g]
            wide = jnp.concatenate([lane_bcast(vals[g], c) for c in cols] + [vals[g]], axis=1)
            spread = {t: [lane_bcast(vals[t], c) for c in cols] for t in others}
            for p in range(SUBL):
                piv, wide = wide[:, :LANES], wide[:, LANES:]
                wide = jnp.minimum(wide, widen(piv, wide.shape[1]) + jnp.broadcast_to(wide[p:p + 1, :], wide.shape))
            vals[g] = wide
            for t in others[g:] + others[:g]:
                for n in range(SUBL):
                    vals[t] = jnp.minimum(vals[t], widen(spread[t][n], own + blk) + jnp.broadcast_to(wide[n:n + 1, :], wide.shape))
        for t, v in enumerate(vals):
            work[tile_rows(base + t, base + t + 1), blk:width] = v
        for c in range(0, own + blk, LANES):
            packed = pack_rows(jnp.concatenate([v[:, c:c + LANES] for v in vals], axis=0))
            for n, v in enumerate(packed):
                r = slice(n * PAIRS, (n + 1) * PAIRS)
                rowp[k, a, r, blk + c:blk + c + LANES] = v
                if c == dl:
                    rowp[k, a, r, 0:blk] = v

    def send_chunk(k, a):
        sends_next = (k + 1 < nrows) & (my_col == (k + 1) % ncols)

        row_copy(k, a, 0).start()
        row_copy(k, a, 2).start()
        row_copy(k, a, 1).start()

        @pl.when(sends_next)
        def _():
            for d in tuple(range(2, ncols - 1)) + (1, ncols - 1):
                nxt_copy(k, a, d).start()

        @pl.when(k + 1 == nrows)
        def _():
            row_copy(k, a, 3).start()

    def relax_by_chunk(a, f, l, step):
        for t in range(f, l, step):
            r = tile_rows(t, min(t + step, l))
            rows = lambda n: work[a * CHUNK + n:a * CHUNK + n + 1, blk:width]
            work[r, blk:width] = relax(work[r, blk:width], work[r, dlo:width], range(a * CHUNK, (a + 1) * CHUNK), rows)

    def spread_cols(a, f, l):
        r = tile_rows(f, l)
        src = work[r, dlo:width]
        for n in range(CHUNK):
            spread[n, r, :] = lane_bcast(src, a * CHUNK + n)

    def relax_spread(a, f, l):
        r = tile_rows(f, l)
        acc = work[r, blk:width]
        for n in range(CHUNK):
            row = work[a * CHUNK + n:a * CHUNK + n + 1, blk:width]
            acc = jnp.minimum(acc, widen(spread[n, r, :], own + blk) + jnp.broadcast_to(row, acc.shape))
        work[r, blk:width] = acc

    def own_turn(k):
        n = tiles_per_chunk

        close_chunk(k, 0)
        spread_cols(0, n, 2 * n)
        send_chunk(k, 0)
        relax_spread(0, n, 2 * n)
        close_chunk(k, 1)
        relax_by_chunk(0, 2 * n, 3 * n, n)
        spread_cols(1, 2 * n, 3 * n)
        relax_by_chunk(0, 3 * n, tiles, n)
        send_chunk(k, 1)
        relax_spread(1, 2 * n, 3 * n)
        close_chunk(k, 2)
        relax_by_chunk(1, 3 * n, tiles, n)
        spread_cols(2, 3 * n, tiles)
        send_chunk(k, 2)
        relax_spread(2, 3 * n, tiles)
        close_chunk(k, 3)
        send_chunk(k, 3)
        for a in range(1, nchunk):
            def body(it, carry):
                r = pl.ds(pl.multiple_of(it * CHUNK, CHUNK), CHUNK)
                rows = lambda n: work[a * CHUNK + n:a * CHUNK + n + 1, blk:width]
                work[r, blk:width] = relax(work[r, blk:width], work[r, dlo:width], range(a * CHUNK, (a + 1) * CHUNK), rows)
                return carry
            lax.fori_loop(0, a, body, 0)

    def recv_row(k, a):
        fwd_copy(k, a).wait_recv()

        @pl.when(fwd_here(k))
        def _():
            fwd_copy(k, a).start()

        @pl.when(far_here(k, a))
        def _():
            far_copy(k, a).start()

    def relax_block(k, chunks, start, count, sections, save=False, load=False):
        chunks = chunks if isinstance(chunks, tuple) else (chunks,)
        low = lane_id(STEP) < LANES // 2
        pairs = pair_lanes(STEP)
        sizes = [c.size if isinstance(c, pl.Slice) else c.stop - c.start for c in sections]
        for i in range(count // STEP):
            r = pl.ds(pl.multiple_of(start + i * STEP, STEP), STEP)
            src = None if load else work[r, 0:blk]
            accs = [None] * len(sections)
            for a, n in [(a, n) for a in chunks for n in range(PAIRS)]:
                if load:
                    wide = spread[a * PAIRS + n, r, :]
                else:
                    wide = pair_bcast(src, pairs + (a * CHUNK + n))
                if save:
                    spread[a * PAIRS + n, r, :] = wide
                for c, (cols, size) in enumerate(zip(sections, sizes)):
                    reps = widen(wide, size)
                    new = [reps + jnp.broadcast_to(rowp[k, a, m:m + 1, cols], reps.shape) for m in (n, n + PAIRS)]
                    accs[c] = new if accs[c] is None else [jnp.minimum(x, y) for x, y in zip(accs[c], new)]
            for (lower, upper), cols in zip(accs, sections):
                parts = []
                for b in range(0, lower.shape[1], LANES):
                    x, y = lower[:, b:b + LANES], upper[:, b:b + LANES]
                    parts.append(jnp.minimum(jnp.where(low, x, y), pltpu.roll(jnp.where(low, y, x), LANES // 2, 1)))
                work[r, cols] = jnp.minimum(work[r, cols], jnp.concatenate(parts, axis=1))


    first = slice(0, blk)

    def rest(k, b):
        other = pl.ds(pl.multiple_of(own - b // ncols * blk, LANES), blk)
        def body(h, carry):
            relax_block(k, tuple(range(nchunk)), h * half, half, [other], load=True)
            return carry
        lax.fori_loop(0, HALVES, body, 0)

    def next_turn(k):
        last = nchunk - 1

        def next_rows(a):
            holder = my_col == (k + 1) % ncols

            @pl.when(holder)
            def _():
                rowp[k, a, :, dlo:width] = rowp[k, a, :, own_cols(k + 1)]

            @pl.when(jnp.logical_not(holder))
            def _():
                nxt_copy(k, a, 1).wait_recv()

        recv_row(k, 0)

        def spread_last(h):
            src = work[half_rows(h), 0:blk]
            pairs = pair_lanes(half)
            for n in range(PAIRS):
                spread[last * PAIRS + n, half_rows(h), :] = pair_bcast(src, pairs + (last * CHUNK + n))

        @pl.when(sub >= 0)
        def _():
            def body(h, carry):
                recv_col(k, h)
                for a in range(last):
                    if a > 0:
                        @pl.when(h == 0)
                        def _():
                            recv_row(k, a)
                    relax_block(k, a, h * half, half, [slice(0, dlo)], save=True)
                spread_last(h)

                @pl.when((h == 0) & (sub == 0))
                def _():
                    recv_row(k, last)
                return carry
            lax.fori_loop(0, HALVES, body, 0)

        @pl.when(sub > 0)
        def _():
            recv_row(k, last)

        def finish(h, carry):
            relax_block(k, last, h * half, half, [slice(blk, dlo)], load=True)
            return carry
        lax.fori_loop(0, HALVES, finish, 0)
        recv_diag()
        for a in range(last):
            next_rows(a)
        relax_block(k, tuple(range(last)), 0, blk, [slice(dlo, width)], load=True)
        next_rows(last)
        relax_block(k, last, 0, blk, [slice(dlo, width)], load=True)

    def second_turn(k):
        sends_col = my_col == (k + 1) % ncols
        sends_diag = my_col == (k + 2) % ncols
        block = jnp.where(sends_col, k + 1, k + 2)
        recv_row(k, 0)

        def half_turn(h, sections, save):
            recv_col(k, h)
            for a in range(nchunk):
                if a > 0:
                    @pl.when(h == 0)
                    def _():
                        recv_row(k, a)
                relax_block(k, a, h * half, half, sections(a), save=save)

        @pl.when(sends_col | sends_diag)
        def _():
            def body(h, carry):
                half_turn(h, lambda a: ([first] if a < nchunk - 1 else []) + [own_cols(block)], True)

                @pl.when(sends_col)
                def _():
                    send_col(k + 1, h)

                @pl.when(sends_diag)
                def _():
                    send_diag(h)
                return carry
            lax.fori_loop(0, HALVES, body, 0)
            rest(k, block)

        @pl.when(jnp.logical_not(sends_col | sends_diag))
        def _():
            def body(h, carry):
                half_turn(h, lambda a: [slice(0 if a < nchunk - 1 else blk, dlo)], False)
                return carry
            lax.fori_loop(0, HALVES, body, 0)

    def store_half(h):
        return pltpu.make_async_copy(work.at[half_rows(h), blk:dlo], out_ref.at[0, half_rows(h)], io_sem.at[h])

    def last_turn(k):
        recv_row(k, 0)

        def body(h, carry):
            recv_col(k, h)
            for a in range(nchunk):
                if a > 0:
                    @pl.when(h == 0)
                    def _():
                        recv_row(k, a)
                relax_block(k, a, h * half, half, [slice(0 if a < nchunk - 1 else blk, dlo)])
            store_half(h).start()
            return carry
        lax.fori_loop(0, HALVES, body, 0)

    def other_turn(k):
        holder = (k + 1 < nrows) & (my_col == (k + 1) % ncols)
        recv_row(k, 0)

        @pl.when(holder)
        def _():
            def body(h, carry):
                recv_col(k, h)
                for a in range(nchunk):
                    if a > 0:
                        @pl.when(h == 0)
                        def _():
                            recv_row(k, a)
                    relax_block(k, a, h * half, half, ([first] if a < nchunk - 1 else []) + [own_cols(k + 1)], save=True)
                send_col(k + 1, h)
                return carry
            lax.fori_loop(0, HALVES, body, 0)
            rest(k, k + 1)

        @pl.when(jnp.logical_not(holder))
        def _():
            def body(h, carry):
                recv_col(k, h)
                for a in range(nchunk):
                    if a > 0:
                        @pl.when(h == 0)
                        def _():
                            recv_row(k, a)
                    relax_block(k, a, h * half, half, [slice(0 if a < nchunk - 1 else blk, dlo)])
                return carry
            lax.fori_loop(0, HALVES, body, 0)

    def round_body(k, carry):
        @pl.when(my_row == k)
        def _():
            @pl.when(k == 0)
            def _():
                recv_diag()
            own_turn(k)

            @pl.when((k + 1 < nrows) & (my_col == (k + 1) % ncols))
            def _():
                for h in range(HALVES):
                    send_col(k + 1, h)

        @pl.when(my_row == k + 1)
        def _():
            next_turn(k)

        @pl.when(my_row == k + 2)
        def _():
            second_turn(k)

        @pl.when(((my_row < k) & (k + 1 < nrows)) | (my_row > k + 2))
        def _():
            other_turn(k)

        @pl.when((my_row < k) & (k + 1 == nrows))
        def _():
            last_turn(k)
        return carry

    lax.fori_loop(0, nrows, round_body, 0)

    @pl.when(my_row + 1 == nrows)
    def _():
        for h in range(HALVES):
            store_half(h).start()

    @pl.when(my_col == my_row % ncols)
    def _():
        for h in range(HALVES):
            for d in range(1, ncols):
                diag_copy(h, d).wait_send()

    def drain(k, carry):
        @pl.when((my_col == k % ncols) & (my_row != k))
        def _():
            for h in range(HALVES):
                for d in range(1, ncols):
                    col_copy(k, h, d, d - 1).wait_send()
        for a in range(nchunk):
            @pl.when(fwd_here(k))
            def _():
                fwd_copy(k, a).wait_send()

            @pl.when(far_here(k, a))
            def _():
                far_copy(k, a).wait_send()
        return carry
    lax.fori_loop(0, nrows, drain, 0)
    for a in range(nchunk):
        for n in range(3):
            row_copy(my_row, a, n).wait_send()

        @pl.when(my_row + 1 == nrows)
        def _():
            row_copy(my_row, a, 3).wait_send()

        @pl.when((my_row + 1 < nrows) & (my_col == (my_row + 1) % ncols))
        def _():
            for d in range(1, ncols):
                nxt_copy(my_row, a, d).wait_send()
    for h in range(HALVES):
        store_half(h).wait()


def solution(mesh):
    nsub = mesh.shape['sub']
    nrows = mesh.shape['row'] * nsub
    ncols = mesh.shape['col']
    dist_spec = P(('parts', 'row', 'sub'), None, 'col')

    def local_run(local):
        rows_local, blk, own = local.shape
        assert rows_local == 1
        nchunk = blk // CHUNK
        nx = nrows // nsub
        dma = pltpu.SemaphoreType.DMA
        vmem = lambda *s: pltpu.VMEM(s, jnp.float32)
        return pl.pallas_call(
            functools.partial(kernel, nrows, ncols, nsub, blk),
            out_shape=jax.ShapeDtypeStruct(local.shape, local.dtype),
            in_specs=[pl.BlockSpec(memory_space=pl.ANY)],
            out_specs=pl.BlockSpec(memory_space=pl.ANY),
            scratch_shapes=[
                vmem(blk, own + 2 * blk), vmem(blk, blk), vmem(nrows, blk, blk),
                vmem(nrows, nchunk, CHUNK, own + 2 * blk), vmem(blk, blk, LANES), dma((HALVES,)),
                dma((nrows, HALVES, ncols - 1)), dma((nrows, HALVES)), dma((HALVES, ncols - 1)), dma((HALVES,)),
                dma((nchunk, 4)), dma((nrows, nchunk)), dma((nrows, nchunk, 2)),
                dma((nchunk, ncols - 1)), dma((nchunk,)),
            ],
            compiler_params=pltpu.CompilerParams(collective_id=0, has_side_effects=True, vmem_limit_bytes=16 * 2**20),
        )(local)

    return jax.shard_map(local_run, mesh=mesh, in_specs=(dist_spec,), out_specs=dist_spec, check_vma=False)
```
